32 devices in a mesh: dp: 2 (over x), sx: 4 (over z), sy: 4 (over y, core).
Axes of the slice: x: 2, y: 2, z: 4, core: 2. Of those that a mesh axis runs over, the one named last changes fastest.
Arguments:
- act_in: bfloat16 [24, 1024, 32, 256], P('dp', 'sy', 'sx'), parts along dimension 0
- norm_first: bfloat16 [2, 256], replicated
- w_first: bfloat16 [3, 3, 256, 128], replicated
- w_short: bfloat16 [256, 128], replicated
- norm_rest: bfloat16 [6, 2, 128], replicated
- w_rest: bfloat16 [5, 3, 3, 128, 128], replicated
- bias_rest: bfloat16 [7, 128], replicated
- w_out: bfloat16 [3, 3, 128, 3], replicated
- bias_out: bfloat16 [3], replicated
Outputs:
- output: float32 [24, 1024, 32, 3], P('dp', 'sy', 'sx'), parts along dimension 0
There are 2 independent parts. The reference program is written for one: setup_inputs(seed, part) draws one part's arguments, and reference() takes and returns one part's arrays. A program takes and returns all parts, laid end to end along the dimension named above; an argument that names none is the same for every part.
All inputs are finite; a program needn't handle non-finite values.
Results may differ from the reference program's by a relative error of at most 0.00909453.
Values are sent between devices in bfloat16 or wider.
A program may use at most 1 GiB of HBM per device.

```python
import math
import jax
import jax.numpy as jnp
from jax import lax

SAMPLES = 12
IMG_H = 1024
IMG_W = 32
IN_CH = 256
MID_CH = 128
OUT_CH = 3
GROUPS = 32
GN_EPS = 1e-6


def normal_weight(key, shape, fan_in):
    return (jax.random.normal(key, shape, jnp.float32) * fan_in ** -0.5).astype(jnp.bfloat16)


def norm_params(key, layer_count, chan_count):
    gain_key, shift_key = jax.random.split(key)
    gains = 1.0 + 0.25 * jax.random.normal(gain_key, (layer_count, chan_count), jnp.float32)
    shifts = 0.25 * jax.random.normal(shift_key, (layer_count, chan_count), jnp.float32)
    return jnp.stack([gains, shifts], axis=1).astype(jnp.bfloat16)


def setup_inputs(seed: int = 0, part: int = 0) -> dict:
    base_key = jax.random.key(seed)
    act_keys = jax.random.split(jax.random.fold_in(base_key, part), 6)
    weight_keys = jax.random.split(base_key, 8)
    wave_count = 3
    base_noise = jax.random.normal(act_keys[0], (SAMPLES, IMG_H, IMG_W, IN_CH), jnp.float32)
    wave_amp = jax.random.normal(act_keys[1], (SAMPLES, wave_count, 1, IN_CH), jnp.float32)
    row_freq = jax.random.uniform(act_keys[2], (SAMPLES, wave_count, 1, 1), jnp.float32, 0.5, 2.5)
    col_freq = jax.random.uniform(act_keys[3], (SAMPLES, wave_count, 1, 1), jnp.float32, 0.5, 2.5)
    row_phase = jax.random.uniform(act_keys[4], (SAMPLES, wave_count, 1, IN_CH), jnp.float32, 0.0, 2.0 * math.pi)
    col_phase = jax.random.uniform(act_keys[5], (SAMPLES, wave_count, 1, IN_CH), jnp.float32, 0.0, 2.0 * math.pi)
    row_pos = (jnp.arange(IMG_H, dtype=jnp.float32) / IMG_H)[:, None]
    col_pos = (jnp.arange(IMG_W, dtype=jnp.float32) / IMG_W)[:, None]
    row_wave = wave_amp * jnp.cos(2.0 * math.pi * row_freq * row_pos + row_phase)
    col_wave = jnp.cos(2.0 * math.pi * col_freq * col_pos + col_phase)
    smooth_field = jnp.einsum("skhc,skwc->shwc", row_wave, col_wave)
    act_in = (0.7 * base_noise + smooth_field).astype(jnp.bfloat16)
    return {
        "act_in": act_in,
        "norm_first": norm_params(weight_keys[0], 1, IN_CH)[0],
        "w_first": normal_weight(weight_keys[1], (3, 3, IN_CH, MID_CH), 9 * IN_CH),
        "w_short": normal_weight(weight_keys[2], (IN_CH, MID_CH), IN_CH),
        "norm_rest": norm_params(weight_keys[3], 6, MID_CH),
        "w_rest": normal_weight(weight_keys[4], (5, 3, 3, MID_CH, MID_CH), 9 * MID_CH),
        "bias_rest": (0.3 * jax.random.normal(weight_keys[5], (7, MID_CH), jnp.float32)).astype(jnp.bfloat16),
        "w_out": normal_weight(weight_keys[6], (3, 3, MID_CH, OUT_CH), 9 * MID_CH),
        "bias_out": (0.3 * jax.random.normal(weight_keys[7], (OUT_CH,), jnp.float32)).astype(jnp.bfloat16),
    }


def group_norm_act(act_map, norm_pair):
    num_rows, num_cols, channels = act_map.shape
    per_group = channels // GROUPS
    group_count = num_rows * num_cols * per_group
    sum_one = jnp.sum(act_map, axis=(0, 1), dtype=jnp.float32).reshape(GROUPS, per_group).sum(axis=1)
    sum_two = jnp.sum(jnp.square(act_map.astype(jnp.float32)), axis=(0, 1)).reshape(GROUPS, per_group).sum(axis=1)
    group_mean = sum_one / group_count
    inv_std = lax.rsqrt(sum_two / group_count - group_mean * group_mean + GN_EPS)
    chan_scale = jnp.repeat(inv_std, per_group) * norm_pair[0].astype(jnp.float32)
    chan_shift = norm_pair[1].astype(jnp.float32) - jnp.repeat(group_mean, per_group) * chan_scale
    return jax.nn.silu(act_map.astype(jnp.float32) * chan_scale + chan_shift).astype(jnp.bfloat16)


def conv_three(act_map, kernel):
    num_rows, num_cols, in_chans = act_map.shape
    padded = jnp.pad(act_map, ((1, 1), (1, 1), (0, 0)))
    accum_sum = jnp.zeros((num_rows * num_cols, kernel.shape[3]), jnp.float32)
    for row_off in range(3):
        for col_off in range(3):
            window = padded[row_off:row_off + num_rows, col_off:col_off + num_cols].reshape(num_rows * num_cols, in_chans)
            accum_sum = accum_sum + jnp.dot(window, kernel[row_off, col_off], preferred_element_type=jnp.float32)
    return accum_sum.reshape(num_rows, num_cols, kernel.shape[3])


def reference(act_in, norm_first, w_first, w_short, norm_rest, w_rest, bias_rest, w_out, bias_out):
    bias_rows = bias_rest.astype(jnp.float32)

    def decode_sample(sample):
        num_rows, num_cols, in_chans = sample.shape
        mid_act = (conv_three(group_norm_act(sample, norm_first), w_first) + bias_rows[0]).astype(jnp.bfloat16)
        skip_path = jnp.dot(sample.reshape(num_rows * num_cols, in_chans), w_short, preferred_element_type=jnp.float32).reshape(num_rows, num_cols, -1) + bias_rows[6]
        hidden = (conv_three(group_norm_act(mid_act, norm_rest[0]), w_rest[0]) + bias_rows[1] + skip_path).astype(jnp.bfloat16)
        for res_index in range(1, 3):
            first_at = 2 * res_index - 1
            mid_act = (conv_three(group_norm_act(hidden, norm_rest[first_at]), w_rest[first_at]) + bias_rows[first_at + 1]).astype(jnp.bfloat16)
            hidden = (conv_three(group_norm_act(mid_act, norm_rest[first_at + 1]), w_rest[first_at + 1]) + bias_rows[first_at + 2] + hidden.astype(jnp.float32)).astype(jnp.bfloat16)
        return conv_three(group_norm_act(hidden, norm_rest[5]), w_out) + bias_out.astype(jnp.float32)

    return lax.map(decode_sample, act_in)
```

```python
import jax
import jax.numpy as jnp
from jax import lax
from jax.experimental import pallas as pl
from jax.experimental.pallas import tpu as pltpu
from jax.sharding import PartitionSpec as P

GROUPS = 32
GN_EPS = 1e-6
MESH = pl.DeviceIdType.MESH
LAG = 4


def solution(mesh):
    rows_n = mesh.shape["sy"]
    cols_n = mesh.shape["sx"]
    tile_spec = P("dp", "sy", "sx", None)
    replicated = P()
    bf16 = jnp.bfloat16
    f32 = jnp.float32

    def make_kernel(samples, tile_h, tile_w):
        lanes = 16
        planes = tile_h // lanes
        ext_w = tile_w + 2
        pairs = planes // 2
        pixel_count = float(tile_h * rows_n * tile_w * cols_n)

        def kernel(act_hbm, params, w_first, w_short, w_rest, w_head, out_ref,
                   a_ext, t_ext, h_ext, a_ud, t_ud, h_ud, act_a, act_m, wp_first, wp_rest,
                   raw, stage_lo, stage_hi, rx1, rx2, rx1a, rx2a,
                   raw_sem, halo_send, halo_recv, st1_send, st1_recv, st2_send, st2_recv):
            my_y = lax.axis_index("sy")
            my_x = lax.axis_index("sx")
            has_up = my_y > 0
            has_down = my_y < rows_n - 1
            has_left = my_x > 0
            has_right = my_x < cols_n - 1

            barrier = pltpu.get_barrier_semaphore()
            for step in range(1, rows_n * cols_n):
                other = lax.rem(my_y * cols_n + my_x + step, rows_n * cols_n)
                pl.semaphore_signal(barrier, inc=1, device_id={"sy": other // cols_n, "sx": lax.rem(other, cols_n)}, device_id_type=MESH)

            def fetch(sample, slot):
                return pltpu.make_async_copy(act_hbm.at[sample], raw.at[slot], raw_sem.at[slot])

            fetch(0, 0).start()

            def pair_weights(dst, src, chans):
                for dc in range(3):
                    for j in range(4):
                        base = (dc * 4 + j) * chans
                        zero = jnp.zeros((chans, 128), bf16)
                        dst[pl.ds(base, chans), 0:128] = src(j, dc) if j < 3 else zero
                        dst[pl.ds(base, chans), 128:256] = src(j - 1, dc) if j > 0 else zero

            pair_weights(wp_first, lambda dr, dc: w_first[dr, dc], 256)

            def pair_rest(index, carry):
                pair_weights(wp_rest.at[index], lambda dr, dc: w_rest[index, dr, dc], 128)
                return carry

            lax.fori_loop(0, 5, pair_rest, 0)

            pl.semaphore_wait(barrier, rows_n * cols_n - 1)

            def halo_copies(ext, ud, parity, sample):
                last = planes - 1
                moves = [
                    (has_left, ext.at[sample, :, 1], ext.at[sample, :, ext_w - 1], my_y, my_x - 1),
                    (has_right, ext.at[sample, :, ext_w - 2], ext.at[sample, :, 0], my_y, my_x + 1),
                    (has_up, ext.at[sample, 0, pl.ds(1, tile_w)], ud.at[1, sample, pl.ds(1, tile_w)], my_y - 1, my_x),
                    (has_down, ext.at[sample, last, pl.ds(1, tile_w)], ud.at[0, sample, pl.ds(1, tile_w)], my_y + 1, my_x),
                    (has_up & has_left, ext.at[sample, 0, 1], ud.at[1, sample, ext_w - 1], my_y - 1, my_x - 1),
                    (has_up & has_right, ext.at[sample, 0, ext_w - 2], ud.at[1, sample, 0], my_y - 1, my_x + 1),
                    (has_down & has_left, ext.at[sample, last, 1], ud.at[0, sample, ext_w - 1], my_y + 1, my_x - 1),
                    (has_down & has_right, ext.at[sample, last, ext_w - 2], ud.at[0, sample, 0], my_y + 1, my_x + 1),
                ]
                return [(cond, pltpu.make_async_remote_copy(
                    src_ref=src, dst_ref=dst, send_sem=halo_send.at[sample, index], recv_sem=halo_recv.at[parity, sample, index],
                    device_id={"sy": to_y, "sx": to_x}, device_id_type=MESH))
                    for index, (cond, src, dst, to_y, to_x) in enumerate(moves)]

            arrivals = [has_right, has_left, has_down, has_up, has_down & has_right, has_down & has_left, has_up & has_right, has_up & has_left]

            def peers(buf, send_sem, recv_sem, parity, sample, along_y):
                mine = my_y if along_y else my_x
                count = rows_n if along_y else cols_n
                copies = []
                for step in range(1, count):
                    to = lax.rem(mine + step, count)
                    copies.append(pltpu.make_async_remote_copy(
                        src_ref=buf.at[parity, sample, mine], dst_ref=buf.at[parity, sample, mine],
                        send_sem=send_sem.at[sample, step], recv_sem=recv_sem.at[parity, sample, step],
                        device_id={"sy": to, "sx": my_x} if along_y else {"sy": my_y, "sx": to}, device_id_type=MESH))
                return copies

            def layer_out(layer):
                if layer == 0:
                    return a_ext, a_ud, 0, rx1a, rx2a
                if layer % 2:
                    return t_ext, t_ud, 1, rx1, rx2
                return h_ext, h_ud, 0, rx1, rx2

            def send_edges(layer, sample):
                ext, ud, parity, sums_one, _ = layer_out(layer)
                for cond, copy in halo_copies(ext, ud, parity, sample):
                    @pl.when(cond)
                    def _(copy=copy):
                        copy.start()
                for copy in peers(sums_one, st1_send, st1_recv, parity, sample, True):
                    copy.start()

            def fold_rows(layer, sample):
                _, _, parity, sums_one, sums_two = layer_out(layer)
                for copy in peers(sums_one, st1_send, st1_recv, parity, sample, True):
                    copy.wait_recv()
                total = sums_one[parity, sample, 0]
                for index in range(1, rows_n):
                    total = total + sums_one[parity, sample, index]
                sums_two[parity, sample, my_x] = total

            def send_rows(layer, sample):
                _, _, parity, _, sums_two = layer_out(layer)
                for copy in peers(sums_two, st2_send, st2_recv, parity, sample, False):
                    copy.start()

            def service(layer, sample):
                @pl.when(sample > 0)
                def _():
                    send_edges(layer, sample - 1)

                @pl.when(sample >= LAG + 1)
                def _():
                    send_rows(layer, sample - LAG - 1)

                @pl.when(sample >= LAG)
                def _():
                    fold_rows(layer, sample - LAG)

                if layer > 0:
                    @pl.when(sample < LAG + 1)
                    def _():
                        send_rows(layer - 1, samples + sample - LAG - 1)

                    @pl.when(sample < LAG)
                    def _():
                        fold_rows(layer - 1, samples + sample - LAG)

            def await_layer(layer, sample):
                ext, ud, parity, sums_one, sums_two = layer_out(layer)
                copies = halo_copies(ext, ud, parity, sample)
                for cond, (_, copy) in zip(arrivals, copies):
                    @pl.when(cond)
                    def _(copy=copy):
                        copy.wait_recv()
                for cond, copy in copies:
                    @pl.when(cond)
                    def _(copy=copy):
                        copy.wait_send()
                for copy in peers(sums_one, st1_send, st1_recv, parity, sample, True):
                    copy.wait_send()
                for copy in peers(sums_two, st2_send, st2_recv, parity, sample, False):
                    copy.wait()

            def group_total(value, per_group):
                lane = lax.broadcasted_iota(jnp.int32, value.shape, 1)
                step = 1
                while step < per_group:
                    ahead = pltpu.roll(value, 128 - step, axis=1)
                    behind = pltpu.roll(value, step, axis=1)
                    value = value + jnp.where(lax.rem(lane, 2 * step) < step, ahead, behind)
                    step *= 2
                return value

            def scale_shift(layer, sample):
                _, _, parity, _, sums_two = layer_out(layer)
                total = sums_two[parity, sample, 0]
                for index in range(1, cols_n):
                    total = total + sums_two[parity, sample, index]
                parts = 2 if layer == 0 else 1
                chans = parts * 128
                per_group = chans // GROUPS
                total = group_total(total, per_group) * (1.0 / (pixel_count * per_group))
                result = []
                for part in range(parts):
                    mean = total[part:part + 1]
                    var = total[parts + part:parts + part + 1] - mean * mean
                    inv = lax.rsqrt(var + GN_EPS)
                    row = part if layer == 0 else 4 + 2 * (layer - 1)
                    gap = 2 if layer == 0 else 1
                    scale = inv * params[row:row + 1, :]
                    shift = params[row + gap:row + gap + 1, :] - mean * scale
                    result.append((0.5 * scale, 0.5 * shift))
                if parts == 1:
                    return result[0]
                return tuple(jnp.concatenate([result[0][i], result[1][i]], axis=1) for i in range(2))

            def activate(layer, sample):
                ext, ud, _, _, _ = layer_out(layer)
                dst = act_a if layer == 0 else act_m
                chans = 256 if layer == 0 else 128
                scale, shift = scale_shift(layer, sample)
                scale3 = scale.reshape(1, 1, chans)
                shift3 = shift.reshape(1, 1, chans)

                def silu(x):
                    half = x.astype(f32) * scale3 + shift3
                    return half + half * jnp.tanh(half)

                for q in range(planes):
                    dst[(q + 1) // 2, (q + 1) % 2, pl.ds(1, tile_w)] = silu(ext[sample, q, pl.ds(1, tile_w)]).astype(bf16)
                for col, cond in ((0, has_left), (ext_w - 1, has_right)):
                    for q in range(planes):
                        value = silu(ext[sample, q, pl.ds(col, 1)])
                        dst[(q + 1) // 2, (q + 1) % 2, pl.ds(col, 1)] = jnp.where(cond, value, 0.0).astype(bf16)
                shape = (ext_w, lanes, chans)
                col_id = lax.broadcasted_iota(jnp.int32, shape, 0)
                row_id = lax.broadcasted_iota(jnp.int32, shape, 1)
                col_lo = jnp.where(has_left, 0, 1)
                col_hi = jnp.where(has_right, ext_w - 1, ext_w - 2)
                in_cols = (col_id >= col_lo) & (col_id <= col_hi)
                for side, cond, near, far, turn, edge in ((0, has_up, planes, 0, 1, 0), (1, has_down, 1, planes + 1, lanes - 1, lanes - 1)):
                    own = pltpu.roll(dst[near // 2, near % 2].astype(f32), turn, axis=1)
                    other = pltpu.roll(silu(ud[side, sample]), turn, axis=1)
                    other = jnp.where(in_cols & cond, other, 0.0)
                    dst[far // 2, far % 2] = jnp.where(row_id == edge, other, own).astype(bf16)

            def convolve(layer, sample):
                src = act_a if layer == 1 else act_m
                chans = 256 if layer == 1 else 128
                ext, _, parity, sums_one, _ = layer_out(layer)
                bias_row = 16 + (layer - 1)
                bias = params[bias_row:bias_row + 1, :]
                if layer == 2:
                    bias = bias + params[22:23, :]
                bias4 = bias.reshape(1, 1, 1, 128)
                weights = wp_first if layer == 1 else wp_rest.at[layer - 2]
                sum_one = jnp.zeros((8, 128), f32)
                sum_two = jnp.zeros((8, 128), f32)
                parts = 2
                span = pairs // parts
                for part in range(parts):
                    pieces = []
                    for dc in range(3):
                        for j in range(4):
                            piece = src[pl.ds(part * span + j // 2, span), j % 2, pl.ds(dc, tile_w)]
                            pieces.append(piece.reshape(span * tile_w * lanes, chans))
                    accum = jnp.dot(jnp.concatenate(pieces, axis=1), weights[...], preferred_element_type=f32)
                    for k in range(span):
                        for odd in range(2):
                            q = 2 * (part * span + k) + odd
                            value = accum[k * 128:(k + 1) * 128, odd * 128:(odd + 1) * 128].reshape(tile_w, lanes, 128) + bias.reshape(1, 1, 128)
                            if layer == 2:
                                skip = jnp.dot(a_ext[sample, q, pl.ds(1, tile_w)].reshape(128, 256), w_short[...], preferred_element_type=f32)
                                value = value + skip.reshape(tile_w, lanes, 128)
                            elif layer % 2 == 0:
                                value = value + ext[sample, q, pl.ds(1, tile_w)].astype(f32)
                            value = value.astype(bf16)
                            ext[sample, q, pl.ds(1, tile_w)] = value
                            wide = value.astype(f32).reshape(tile_w * 2, 8, 128)
                            sum_one = sum_one + jnp.sum(wide, axis=0)
                            sum_two = sum_two + jnp.sum(wide * wide, axis=0)
                sums_one[parity, sample, my_y] = jnp.concatenate(
                    [jnp.sum(sum_one, axis=0, keepdims=True), jnp.sum(sum_two, axis=0, keepdims=True)], axis=0)

            def load_step(sample, carry):
                slot = lax.rem(sample, 2)
                fetch(sample, slot).wait()

                @pl.when(sample + 1 < samples)
                def _():
                    fetch(sample + 1, 1 - slot).start()

                service(0, sample)
                for chunk in range(tile_h // 16):
                    piece = raw[slot, pl.ds(chunk * 16, 16)].astype(f32).reshape(16 * tile_w, 256)
                    stage_lo[pl.ds(chunk * 16 * tile_w, 16 * tile_w), :] = piece[:, :128]
                    stage_hi[pl.ds(chunk * 16 * tile_w, 16 * tile_w), :] = piece[:, 128:]
                for half, stage in ((0, stage_lo), (1, stage_hi)):
                    sum_one = jnp.zeros((lanes, 128), f32)
                    sum_two = jnp.zeros((lanes, 128), f32)
                    for q in range(planes):
                        for c in range(tile_w):
                            value = stage[pl.ds(q * tile_w + c, lanes, stride=planes * tile_w), :]
                            a_ext[sample, q, c + 1, :, half * 128:(half + 1) * 128] = value.astype(bf16)
                            sum_one = sum_one + value
                            sum_two = sum_two + value * value
                    rx1a[0, sample, my_y, half:half + 1] = jnp.sum(sum_one, axis=0, keepdims=True)
                    rx1a[0, sample, my_y, half + 2:half + 3] = jnp.sum(sum_two, axis=0, keepdims=True)
                return carry

            lax.fori_loop(0, samples, load_step, 0)
            send_edges(0, samples - 1)

            for layer in range(1, 7):
                def conv_step(sample, carry, layer=layer):
                    service(layer, sample)
                    await_layer(layer - 1, sample)
                    activate(layer - 1, sample)
                    convolve(layer, sample)
                    return carry

                lax.fori_loop(0, samples, conv_step, 0)
                send_edges(layer, samples - 1)

            def head_step(sample, carry):
                @pl.when(sample < LAG + 1)
                def _():
                    send_rows(6, samples + sample - LAG - 1)

                @pl.when(sample < LAG)
                def _():
                    fold_rows(6, samples + sample - LAG)

                await_layer(6, sample)
                activate(6, sample)
                flat = act_m[...].reshape((planes + 2) * ext_w * lanes, 128)
                width = out_ref.shape[2]
                flat = jnp.concatenate([flat, jnp.zeros((width - flat.shape[0], 128), bf16)], axis=0)
                taps = lax.dot_general(w_head[...], flat, (((1,), (1,)), ((), ())), preferred_element_type=f32)
                image = taps[0:8]
                for tap in range(1, 9):
                    offset = ((tap // 3) * ext_w + tap % 3) * lanes
                    image = image + pltpu.roll(taps[8 * tap:8 * tap + 8], width - offset, axis=1)
                out_ref[sample] = image
                return carry

            lax.fori_loop(0, samples, head_step, 0)

        return kernel, lanes, planes, ext_w

    def local_decode(act_in, norm_first, w_first, w_short, norm_rest, w_rest, bias_rest, w_out, bias_out):
        samples, tile_h, tile_w, _ = act_in.shape
        kernel, lanes, planes, ext_w = make_kernel(samples, tile_h, tile_w)
        params = jnp.concatenate([norm_first.reshape(4, 128), norm_rest.reshape(12, 128), bias_rest, jnp.zeros((1, 128), bf16)], axis=0).astype(f32)
        w_head = jnp.pad(w_out.transpose(0, 1, 3, 2).reshape(9, 3, 128), ((0, 0), (0, 5), (0, 0))).reshape(72, 128)
        width = -(-((planes + 2) * ext_w * lanes) // 128) * 128
        vmem = pl.BlockSpec(memory_space=pltpu.VMEM)
        scratch = [
            pltpu.VMEM((samples, planes, ext_w, lanes, 256), bf16),
            pltpu.VMEM((samples, planes, ext_w, lanes, 128), bf16),
            pltpu.VMEM((samples, planes, ext_w, lanes, 128), bf16),
            pltpu.VMEM((2, samples, ext_w, lanes, 256), bf16),
            pltpu.VMEM((2, samples, ext_w, lanes, 128), bf16),
            pltpu.VMEM((2, samples, ext_w, lanes, 128), bf16),
            pltpu.VMEM(((planes + 2) // 2, 2, ext_w, lanes, 256), bf16),
            pltpu.VMEM(((planes + 2) // 2, 2, ext_w, lanes, 128), bf16),
            pltpu.VMEM((12 * 256, 256), bf16),
            pltpu.VMEM((5, 12 * 128, 256), bf16),
            pltpu.VMEM((2, tile_h, tile_w, 256), bf16),
            pltpu.VMEM((tile_h * tile_w, 128), f32),
            pltpu.VMEM((tile_h * tile_w, 128), f32),
            pltpu.VMEM((2, samples, rows_n, 2, 128), f32),
            pltpu.VMEM((2, samples, cols_n, 2, 128), f32),
            pltpu.VMEM((1, samples, rows_n, 4, 128), f32),
            pltpu.VMEM((1, samples, cols_n, 4, 128), f32),
            pltpu.SemaphoreType.DMA((2,)),
            pltpu.SemaphoreType.DMA((samples, 8)),
            pltpu.SemaphoreType.DMA((2, samples, 8)),
            pltpu.SemaphoreType.DMA((samples, rows_n)),
            pltpu.SemaphoreType.DMA((2, samples, rows_n)),
            pltpu.SemaphoreType.DMA((samples, cols_n)),
            pltpu.SemaphoreType.DMA((2, samples, cols_n)),
        ]
        image = pl.pallas_call(
            kernel,
            out_shape=jax.ShapeDtypeStruct((samples, 8, width), f32),
            in_specs=[pl.BlockSpec(memory_space=pl.ANY), vmem, vmem, vmem, vmem, vmem],
            out_specs=vmem,
            scratch_shapes=scratch,
            compiler_params=pltpu.CompilerParams(collective_id=0, has_side_effects=True, vmem_limit_bytes=60 * 1024 * 1024),
        )(act_in, params, w_first, w_short, w_rest, w_head)
        image = image[:, :3, :planes * ext_w * lanes].reshape(samples, 3, planes, ext_w, lanes)[:, :, :, :tile_w]
        image = image.transpose(0, 4, 2, 3, 1).reshape(samples, tile_h, tile_w, 3)
        return image + bias_out.astype(f32)

    return jax.shard_map(local_decode, mesh=mesh, in_specs=(tile_spec, replicated, replicated, replicated, replicated, replicated, replicated, replicated, replicated), out_specs=tile_spec, check_vma=False)
```

```python
import jax
import jax.numpy as jnp
from jax import lax
from jax.experimental import pallas as pl
from jax.experimental.pallas import tpu as pltpu
from jax.sharding import PartitionSpec as P

GROUPS = 32
GN_EPS = 1e-6
MESH = pl.DeviceIdType.MESH
BATCH = 3


def solution(mesh):
    rows_n = mesh.shape["sy"]
    cols_n = mesh.shape["sx"]
    tile_spec = P("dp", "sy", "sx", None)
    replicated = P()
    bf16 = jnp.bfloat16
    f32 = jnp.float32

    def make_kernel(samples, tile_h, tile_w):
        lanes = 16
        planes = tile_h // lanes
        ext_w = tile_w + 2
        pairs = planes // 2
        pixel_count = float(tile_h * rows_n * tile_w * cols_n)

        batches = samples // BATCH
        column_lanes = (planes + 2) * lanes
        flat_width = -(-(ext_w * column_lanes) // 128) * 128

        def kernel(act_hbm, norm_first, norm_rest, bias_rest, bias_out, w_first, w_short, w_rest, w_out, out_ref,
                   a_ext, t_ext, h_ext, a_ud, t_ud, h_ud, act_a, act_m, wp_first, wp_rest, w_head, reorder, image_rows,
                   raw, stage_lo, stage_hi, rx1, rx2, rx1a, rx2a,
                   raw_sem, col_send, col_recv, row_send, row_recv, st1_send, st1_recv, st2_send, st2_recv):
            my_y = lax.axis_index("sy")
            my_x = lax.axis_index("sx")
            has_up = my_y > 0
            has_down = my_y < rows_n - 1
            has_left = my_x > 0
            has_right = my_x < cols_n - 1

            barrier = pltpu.get_barrier_semaphore()
            for step in range(1, rows_n * cols_n):
                other = lax.rem(my_y * cols_n + my_x + step, rows_n * cols_n)
                pl.semaphore_signal(barrier, inc=1, device_id={"sy": other // cols_n, "sx": lax.rem(other, cols_n)}, device_id_type=MESH)

            def fetch(sample, slot):
                return pltpu.make_async_copy(act_hbm.at[sample], raw.at[slot], raw_sem.at[slot])

            fetch(0, 0).start()

            def pair_weights(dst, src, chans):
                for dc in range(3):
                    for j in range(4):
                        base = (dc * 4 + j) * chans
                        zero = jnp.zeros((chans, 128), bf16)
                        dst[pl.ds(base, chans), 0:128] = src(j, dc) if j < 3 else zero
                        dst[pl.ds(base, chans), 128:256] = src(j - 1, dc) if j > 0 else zero

            pair_weights(wp_first, lambda dr, dc: w_first[dr, dc], 256)

            def pair_rest(index, carry):
                pair_weights(wp_rest.at[index], lambda dr, dc: w_rest[index, dr, dc], 128)
                return carry

            lax.fori_loop(0, 5, pair_rest, 0)

            for tap in range(9):
                taps3 = w_out[tap // 3, tap % 3].astype(f32)
                w_head[pl.ds(8 * tap, 8), :] = jnp.concatenate([taps3, jnp.zeros((5, 128), f32)], axis=0)
            from_id = lax.broadcasted_iota(jnp.int32, (tile_h, tile_h), 0)
            to_id = lax.broadcasted_iota(jnp.int32, (tile_h, tile_h), 1)
            reorder[...] = jnp.where(lax.rem(from_id, lanes) * planes + from_id // lanes == to_id, 1.0, 0.0).astype(bf16)

            pl.semaphore_wait(barrier, rows_n * cols_n - 1)

            def span(batch):
                return pl.ds(batch * BATCH, BATCH)

            def remote(src, dst, send_sem, recv_sem, to_y, to_x):
                return pltpu.make_async_remote_copy(src_ref=src, dst_ref=dst, send_sem=send_sem, recv_sem=recv_sem,
                                                    device_id={"sy": to_y, "sx": to_x}, device_id_type=MESH)

            def column_copies(ext, parity, sample):
                moves = [(has_left, has_right, 1, ext_w - 1, my_x - 1), (has_right, has_left, ext_w - 2, 0, my_x + 1)]
                return [(leaves, arrives, remote(ext.at[sample, :, src], ext.at[sample, :, dst], col_send.at[sample, index], col_recv.at[parity, sample, index], my_y, to_x))
                        for index, (leaves, arrives, src, dst, to_x) in enumerate(moves)]

            def row_copies(ext, ud, parity, batch):
                moves = [(has_up, has_down, 0, 1, my_y - 1), (has_down, has_up, planes - 1, 0, my_y + 1)]
                return [(leaves, arrives, remote(ext.at[span(batch), src], ud.at[side, span(batch)], row_send.at[batch, side], row_recv.at[parity, batch, side], to_y, my_x))
                        for leaves, arrives, src, side, to_y in moves]

            def peers(buf, send_sem, recv_sem, parity, batch, along_y):
                mine = my_y if along_y else my_x
                count = rows_n if along_y else cols_n
                copies = []
                for step in range(1, count):
                    to = lax.rem(mine + step, count)
                    slot = buf.at[parity, batch, mine]
                    copies.append(remote(slot, slot, send_sem.at[batch, step], recv_sem.at[parity, batch, step], to if along_y else my_y, my_x if along_y else to))
                return copies

            def layer_out(layer):
                if layer == 0:
                    return a_ext, a_ud, 0, rx1a, rx2a
                if layer % 2:
                    return t_ext, t_ud, 1, rx1, rx2
                return h_ext, h_ud, 0, rx1, rx2

            def start_if(cond, copy):
                @pl.when(cond)
                def _():
                    copy.start()

            def send_columns(layer, sample):
                ext, _, parity, _, _ = layer_out(layer)
                for leaves, _, copy in column_copies(ext, parity, sample):
                    start_if(leaves, copy)

            def send_sums(layer, batch):
                _, _, parity, sums_one, _ = layer_out(layer)
                for copy in peers(sums_one, st1_send, st1_recv, parity, batch, True):
                    copy.start()

            def pass_on(layer, batch):
                ext, ud, parity, sums_one, sums_two = layer_out(layer)
                for index in range(BATCH):
                    for _, arrives, copy in column_copies(ext, parity, batch * BATCH + index):
                        @pl.when(arrives)
                        def _(copy=copy):
                            copy.wait_recv()
                for leaves, _, copy in row_copies(ext, ud, parity, batch):
                    start_if(leaves, copy)
                for copy in peers(sums_one, st1_send, st1_recv, parity, batch, True):
                    copy.wait_recv()
                total = sums_one[parity, batch, 0]
                for index in range(1, rows_n):
                    total = total + sums_one[parity, batch, index]
                parts = 2 if layer == 0 else 1
                for index in range(BATCH):
                    sums_two[parity, batch, my_x, index] = pack_groups(total[index], parts)

            def send_totals(layer, batch):
                _, _, parity, _, sums_two = layer_out(layer)
                for copy in peers(sums_two, st2_send, st2_recv, parity, batch, False):
                    copy.start()

            def boundary(layer, batch):
                @pl.when(batch > 0)
                def _():
                    send_sums(layer, batch - 1)

                @pl.when(batch >= 2)
                def _():
                    pass_on(layer, batch - 2)

                if layer > 0:
                    @pl.when(batch < 2)
                    def _():
                        pass_on(layer - 1, batches + batch - 2)

            def within(layer, batch, index):
                @pl.when((index == 1) & (batch >= 2))
                def _():
                    send_totals(layer, batch - 2)

                if layer > 0:
                    @pl.when((index == 1) & (batch < 2))
                    def _():
                        send_totals(layer - 1, batches + batch - 2)

            def await_batch(layer, batch):
                ext, ud, parity, sums_one, sums_two = layer_out(layer)
                rows = row_copies(ext, ud, parity, batch)
                for _, arrives, copy in rows:
                    @pl.when(arrives)
                    def _(copy=copy):
                        copy.wait_recv()
                for leaves, _, copy in rows:
                    @pl.when(leaves)
                    def _(copy=copy):
                        copy.wait_send()
                for index in range(BATCH):
                    for leaves, _, copy in column_copies(ext, parity, batch * BATCH + index):
                        @pl.when(leaves)
                        def _(copy=copy):
                            copy.wait_send()
                for copy in peers(sums_one, st1_send, st1_recv, parity, batch, True):
                    copy.wait_send()
                for copy in peers(sums_two, st2_send, st2_recv, parity, batch, False):
                    copy.wait()

            def group_total(value, per_group):
                lane = lax.broadcasted_iota(jnp.int32, value.shape, 1)
                step = 1
                while step < per_group:
                    ahead = pltpu.roll(value, 128 - step, axis=1)
                    behind = pltpu.roll(value, step, axis=1)
                    value = value + jnp.where(lax.rem(lane, 2 * step) < step, ahead, behind)
                    step *= 2
                return value

            def pack_groups(sums, parts):
                rows = 2 * parts
                groups = group_total(sums, 128 * parts // GROUPS)
                lane = lax.rem(lax.broadcasted_iota(jnp.int32, (1, 128), 1), rows)
                packed = groups[0:1]
                for row in range(1, rows):
                    packed = jnp.where(lane == row, groups[row:row + 1], packed)
                return packed

            def unpack_groups(packed, parts):
                rows = 2 * parts
                lane = lax.rem(lax.broadcasted_iota(jnp.int32, (1, 128), 1), rows)
                return [group_total(jnp.where(lane == row, packed, 0.0), rows) for row in range(rows)]

            def scale_shift(layer, sample):
                _, _, parity, _, sums_two = layer_out(layer)
                batch, index = sample // BATCH, lax.rem(sample, BATCH)
                total = sums_two[parity, batch, 0, index]
                for source in range(1, cols_n):
                    total = total + sums_two[parity, batch, source, index]
                parts = 2 if layer == 0 else 1
                moments = unpack_groups(total * (1.0 / (pixel_count * (128 * parts // GROUPS))), parts)
                pair = (norm_first[...] if layer == 0 else norm_rest[layer - 1]).astype(f32)
                result = []
                for part in range(parts):
                    mean, square = moments[part], moments[parts + part]
                    inv = lax.rsqrt(square - mean * mean + GN_EPS)
                    scale = inv * pair[0:1, part * 128:(part + 1) * 128]
                    shift = pair[1:2, part * 128:(part + 1) * 128] - mean * scale
                    result.append((0.5 * scale, 0.5 * shift))
                if parts == 1:
                    return result[0]
                return tuple(jnp.concatenate([result[0][i], result[1][i]], axis=1) for i in range(2))

            def activate(layer, sample):
                ext, ud, _, _, _ = layer_out(layer)
                dst = act_a if layer == 0 else act_m
                chans = 256 if layer == 0 else 128
                scale, shift = scale_shift(layer, sample)
                scale3 = scale.reshape(1, 1, chans)
                shift3 = shift.reshape(1, 1, chans)

                def silu(x):
                    half = x.astype(f32) * scale3 + shift3
                    return half + half * jnp.tanh(half)

                for q in range(planes):
                    dst[(q + 1) // 2, (q + 1) % 2, pl.ds(1, tile_w)] = silu(ext[sample, q, pl.ds(1, tile_w)]).astype(bf16)
                for col, cond in ((0, has_left), (ext_w - 1, has_right)):
                    for q in range(planes):
                        value = silu(ext[sample, q, pl.ds(col, 1)])
                        dst[(q + 1) // 2, (q + 1) % 2, pl.ds(col, 1)] = jnp.where(cond, value, 0.0).astype(bf16)
                shape = (ext_w, lanes, chans)
                col_id = lax.broadcasted_iota(jnp.int32, shape, 0)
                row_id = lax.broadcasted_iota(jnp.int32, shape, 1)
                col_lo = jnp.where(has_left, 0, 1)
                col_hi = jnp.where(has_right, ext_w - 1, ext_w - 2)
                in_cols = (col_id >= col_lo) & (col_id <= col_hi)
                for side, cond, near, far, turn, edge in ((0, has_up, planes, 0, 1, 0), (1, has_down, 1, planes + 1, lanes - 1, lanes - 1)):
                    own = pltpu.roll(dst[near // 2, near % 2].astype(f32), turn, axis=1)
                    other = pltpu.roll(silu(ud[side, sample]), turn, axis=1)
                    other = jnp.where(in_cols & cond, other, 0.0)
                    dst[far // 2, far % 2] = jnp.where(row_id == edge, other, own).astype(bf16)

            def convolve(layer, sample):
                src = act_a if layer == 1 else act_m
                chans = 256 if layer == 1 else 128
                ext, _, parity, sums_one, _ = layer_out(layer)
                bias_rows = bias_rest[...].astype(f32)
                bias = bias_rows[layer - 1:layer]
                if layer == 2:
                    bias = bias + bias_rows[6:7]
                weights = wp_first if layer == 1 else wp_rest.at[layer - 2]
                sum_one = jnp.zeros((8, 128), f32)
                sum_two = jnp.zeros((8, 128), f32)
                parts = 2
                half = pairs // parts
                for part in range(parts):
                    pieces = []
                    for dc in range(3):
                        for j in range(4):
                            piece = src[pl.ds(part * half + j // 2, half), j % 2, pl.ds(dc, tile_w)]
                            pieces.append(piece.reshape(half * tile_w * lanes, chans))
                    accum = jnp.dot(jnp.concatenate(pieces, axis=1), weights[...], preferred_element_type=f32)
                    for k in range(half):
                        for odd in range(2):
                            q = 2 * (part * half + k) + odd
                            value = accum[k * 128:(k + 1) * 128, odd * 128:(odd + 1) * 128].reshape(tile_w, lanes, 128) + bias.reshape(1, 1, 128)
                            if layer == 2:
                                skip = jnp.dot(a_ext[sample, q, pl.ds(1, tile_w)].reshape(128, 256), w_short[...], preferred_element_type=f32)
                                value = value + skip.reshape(tile_w, lanes, 128)
                            elif layer % 2 == 0:
                                value = value + ext[sample, q, pl.ds(1, tile_w)].astype(f32)
                            value = value.astype(bf16)
                            ext[sample, q, pl.ds(1, tile_w)] = value
                            wide = value.astype(f32).reshape(tile_w * 2, 8, 128)
                            sum_one = sum_one + jnp.sum(wide, axis=0)
                            sum_two = sum_two + jnp.sum(wide * wide, axis=0)
                sums_one[parity, sample // BATCH, my_y, lax.rem(sample, BATCH)] = jnp.concatenate(
                    [jnp.sum(sum_one, axis=0, keepdims=True), jnp.sum(sum_two, axis=0, keepdims=True)], axis=0)

            def load_step(index, batch):
                sample = batch * BATCH + index
                slot = lax.rem(sample, 2)
                fetch(sample, slot).wait()

                @pl.when(sample + 1 < samples)
                def _():
                    fetch(sample + 1, 1 - slot).start()

                @pl.when(sample > 0)
                def _():
                    send_columns(0, sample - 1)

                within(0, batch, index)
                for chunk in range(tile_h // 16):
                    piece = raw[slot, pl.ds(chunk * 16, 16)].astype(f32).reshape(16 * tile_w, 256)
                    stage_lo[pl.ds(chunk * 16 * tile_w, 16 * tile_w), :] = piece[:, :128]
                    stage_hi[pl.ds(chunk * 16 * tile_w, 16 * tile_w), :] = piece[:, 128:]
                for half, stage in ((0, stage_lo), (1, stage_hi)):
                    sum_one = jnp.zeros((lanes, 128), f32)
                    sum_two = jnp.zeros((lanes, 128), f32)
                    for q in range(planes):
                        for c in range(tile_w):
                            value = stage[pl.ds(q * tile_w + c, lanes, stride=planes * tile_w), :]
                            a_ext[sample, q, c + 1, :, half * 128:(half + 1) * 128] = value.astype(bf16)
                            sum_one = sum_one + value
                            sum_two = sum_two + value * value
                    rx1a[0, sample // BATCH, my_y, lax.rem(sample, BATCH), half:half + 1] = jnp.sum(sum_one, axis=0, keepdims=True)
                    rx1a[0, sample // BATCH, my_y, lax.rem(sample, BATCH), half + 2:half + 3] = jnp.sum(sum_two, axis=0, keepdims=True)
                return batch

            def load_batch(batch, carry):
                boundary(0, batch)
                lax.fori_loop(0, BATCH, load_step, batch)
                return carry

            lax.fori_loop(0, batches, load_batch, 0)
            send_columns(0, samples - 1)
            send_sums(0, batches - 1)

            for layer in range(1, 7):
                def conv_step(index, batch, layer=layer):
                    sample = batch * BATCH + index

                    @pl.when(sample > 0)
                    def _():
                        send_columns(layer, sample - 1)

                    within(layer, batch, index)
                    activate(layer - 1, sample)
                    convolve(layer, sample)
                    return batch

                def conv_batch(batch, carry, layer=layer, conv_step=conv_step):
                    boundary(layer, batch)
                    await_batch(layer - 1, batch)
                    lax.fori_loop(0, BATCH, conv_step, batch)
                    return carry

                lax.fori_loop(0, batches, conv_batch, 0)
                send_columns(layer, samples - 1)
                send_sums(layer, batches - 1)

            def head_step(index, batch):
                sample = batch * BATCH + index

                @pl.when((index == 1) & (batch < 2))
                def _():
                    send_totals(6, batches + batch - 2)

                activate(6, sample)
                flat = jnp.swapaxes(act_m[...].reshape(planes + 2, ext_w, lanes, 128), 0, 1).reshape(ext_w * column_lanes, 128)
                flat = jnp.concatenate([flat, jnp.zeros((flat_width - flat.shape[0], 128), bf16)], axis=0)
                taps = lax.dot_general(w_head[...].astype(bf16), flat, (((1,), (1,)), ((), ())), preferred_element_type=f32)
                image = taps[0:8]
                for tap in range(1, 9):
                    offset = (tap % 3) * column_lanes + (tap // 3) * lanes
                    image = image + pltpu.roll(taps[8 * tap:8 * tap + 8], flat_width - offset, axis=1)
                rest = jnp.concatenate([image[:, c * column_lanes:c * column_lanes + tile_h] for c in range(tile_w)], axis=0)
                moved = jnp.zeros(rest.shape, f32)
                for _ in range(3):
                    piece = rest.astype(bf16)
                    moved = moved + jnp.dot(piece, reorder[...], preferred_element_type=f32)
                    rest = rest - piece.astype(f32)
                for side in range(tile_h // 128):
                    image_rows[side] = moved[:, side * 128:(side + 1) * 128]
                for chan in range(3):
                    for side in range(tile_h // 128):
                        out_ref[sample, chan, :, side * 128:(side + 1) * 128] = image_rows[side, pl.ds(chan, tile_w, stride=8), :] + bias_out[chan]
                return batch

            def head_batch(batch, carry):
                @pl.when(batch < 2)
                def _():
                    pass_on(6, batches + batch - 2)

                await_batch(6, batch)
                lax.fori_loop(0, BATCH, head_step, batch)
                return carry

            lax.fori_loop(0, batches, head_batch, 0)

        return kernel, lanes, planes, ext_w

    def local_decode(act_in, norm_first, w_first, w_short, norm_rest, w_rest, bias_rest, w_out, bias_out):
        samples, tile_h, tile_w, _ = act_in.shape
        kernel, lanes, planes, ext_w = make_kernel(samples, tile_h, tile_w)
        batches = samples // BATCH
        vmem = pl.BlockSpec(memory_space=pltpu.VMEM)
        scratch = [
            pltpu.VMEM((samples, planes, ext_w, lanes, 256), bf16),
            pltpu.VMEM((samples, planes, ext_w, lanes, 128), bf16),
            pltpu.VMEM((samples, planes, ext_w, lanes, 128), bf16),
            pltpu.VMEM((2, samples, ext_w, lanes, 256), bf16),
            pltpu.VMEM((2, samples, ext_w, lanes, 128), bf16),
            pltpu.VMEM((2, samples, ext_w, lanes, 128), bf16),
            pltpu.VMEM(((planes + 2) // 2, 2, ext_w, lanes, 256), bf16),
            pltpu.VMEM(((planes + 2) // 2, 2, ext_w, lanes, 128), bf16),
            pltpu.VMEM((12 * 256, 256), bf16),
            pltpu.VMEM((5, 12 * 128, 256), bf16),
            pltpu.VMEM((72, 128), f32),
            pltpu.VMEM((tile_h, tile_h), bf16),
            pltpu.VMEM((tile_h // 128, 8 * tile_w, 128), f32),
            pltpu.VMEM((2, tile_h, tile_w, 256), bf16),
            pltpu.VMEM((tile_h * tile_w, 128), f32),
            pltpu.VMEM((tile_h * tile_w, 128), f32),
            pltpu.VMEM((2, batches, rows_n, BATCH, 2, 128), f32),
            pltpu.VMEM((2, batches, cols_n, BATCH, 1, 128), f32),
            pltpu.VMEM((1, batches, rows_n, BATCH, 4, 128), f32),
            pltpu.VMEM((1, batches, cols_n, BATCH, 1, 128), f32),
            pltpu.SemaphoreType.DMA((2,)),
            pltpu.SemaphoreType.DMA((samples, 2)),
            pltpu.SemaphoreType.DMA((2, samples, 2)),
            pltpu.SemaphoreType.DMA((batches, 2)),
            pltpu.SemaphoreType.DMA((2, batches, 2)),
            pltpu.SemaphoreType.DMA((batches, rows_n)),
            pltpu.SemaphoreType.DMA((2, batches, rows_n)),
            pltpu.SemaphoreType.DMA((batches, cols_n)),
            pltpu.SemaphoreType.DMA((2, batches, cols_n)),
        ]
        image = pl.pallas_call(
            kernel,
            out_shape=jax.ShapeDtypeStruct((samples, 3, tile_w, tile_h), f32),
            in_specs=[pl.BlockSpec(memory_space=pl.ANY), vmem, vmem, vmem, pl.BlockSpec(memory_space=pltpu.SMEM), vmem, vmem, vmem, vmem],
            out_specs=vmem,
            scratch_shapes=scratch,
            compiler_params=pltpu.CompilerParams(collective_id=0, has_side_effects=True, vmem_limit_bytes=60 * 1024 * 1024),
        )(act_in, norm_first, norm_rest, bias_rest, bias_out.astype(f32), w_first, w_short, w_rest, w_out.transpose(0, 1, 3, 2))
        return image.transpose(0, 3, 2, 1)

    return jax.shard_map(local_decode, mesh=mesh, in_specs=(tile_spec, replicated, replicated, replicated, replicated, replicated, replicated, replicated, replicated), out_specs=tile_spec, check_vma=False)
```

```python
import jax
import jax.numpy as jnp
from jax import lax
from jax.experimental import pallas as pl
from jax.experimental.pallas import tpu as pltpu
from jax.sharding import PartitionSpec as P

GROUPS = 32
GN_EPS = 1e-6
MESH = pl.DeviceIdType.MESH
BATCH = 3


def solution(mesh):
    rows_n = mesh.shape["sy"]
    cols_n = mesh.shape["sx"]
    tile_spec = P("dp", "sy", "sx", None)
    replicated = P()
    bf16 = jnp.bfloat16
    f32 = jnp.float32

    def make_kernel(samples, tile_h, tile_w):
        lanes = 16
        planes = tile_h // lanes
        ext_w = tile_w + 2
        pairs = planes // 2
        pixel_count = float(tile_h * rows_n * tile_w * cols_n)

        batches = samples // BATCH
        column_lanes = (planes + 2) * lanes
        flat_width = -(-(ext_w * column_lanes) // 128) * 128

        def kernel(act_hbm, norm_first, norm_rest, bias_rest, bias_out, w_first_hbm, w_short, w_rest_hbm, w_out, out_ref,
                   a_ext, t_ext, h_ext, a_ud, t_ud, h_ud, act_a0, act_a1, act_m0, act_m1, w_first, w_rest, wp_first, wp_rest, w_head, reorder, image_rows,
                   raw, stage_lo, stage_hi, rx1, rx2, rx1a, rx2a,
                   raw_sem, weight_sem, col_send, col_recv, row_send, row_recv, st1_send, st1_recv, st2_send, st2_recv):
            my_y = lax.axis_index("sy")
            my_x = lax.axis_index("sx")
            has_up = my_y > 0
            has_down = my_y < rows_n - 1
            has_left = my_x > 0
            has_right = my_x < cols_n - 1

            barrier = pltpu.get_barrier_semaphore()
            for step in range(1, rows_n * cols_n):
                other = lax.rem(my_y * cols_n + my_x + step, rows_n * cols_n)
                pl.semaphore_signal(barrier, inc=1, device_id={"sy": other // cols_n, "sx": lax.rem(other, cols_n)}, device_id_type=MESH)

            def fetch(sample, slot):
                return pltpu.make_async_copy(act_hbm.at[sample], raw.at[slot], raw_sem.at[slot])

            first_in = pltpu.make_async_copy(w_first_hbm, w_first, weight_sem.at[0])
            rest_in = pltpu.make_async_copy(w_rest_hbm, w_rest, weight_sem.at[1])
            fetch(0, 0).start()
            first_in.start()
            rest_in.start()
            pl.semaphore_wait(barrier, rows_n * cols_n - 1)

            def pair_weights(dst, src, chans):
                for dc in range(3):
                    for j in range(4):
                        base = (dc * 4 + j) * chans
                        zero = jnp.zeros((chans, 128), bf16)
                        dst[pl.ds(base, chans), 0:128] = src(j, dc) if j < 3 else zero
                        dst[pl.ds(base, chans), 128:256] = src(j - 1, dc) if j > 0 else zero

            def span(batch):
                return pl.ds(batch * BATCH, BATCH)

            def remote(src, dst, send_sem, recv_sem, to_y, to_x):
                return pltpu.make_async_remote_copy(src_ref=src, dst_ref=dst, send_sem=send_sem, recv_sem=recv_sem,
                                                    device_id={"sy": to_y, "sx": to_x}, device_id_type=MESH)

            def column_copies(ext, parity, sample):
                moves = [(has_left, has_right, 1, ext_w - 1, my_x - 1), (has_right, has_left, ext_w - 2, 0, my_x + 1)]
                return [(leaves, arrives, remote(ext.at[sample, :, src], ext.at[sample, :, dst], col_send.at[sample, index], col_recv.at[parity, sample, index], my_y, to_x))
                        for index, (leaves, arrives, src, dst, to_x) in enumerate(moves)]

            def row_copies(ext, ud, parity, batch):
                moves = [(has_up, has_down, 0, 1, my_y - 1), (has_down, has_up, planes - 1, 0, my_y + 1)]
                return [(leaves, arrives, remote(ext.at[span(batch), src], ud.at[side, span(batch)], row_send.at[batch, side], row_recv.at[parity, batch, side], to_y, my_x))
                        for leaves, arrives, src, side, to_y in moves]

            def peers(buf, send_sem, recv_sem, parity, batch, along_y):
                mine = my_y if along_y else my_x
                count = rows_n if along_y else cols_n
                copies = []
                for step in range(1, count):
                    to = lax.rem(mine + step, count)
                    slot = buf.at[parity, batch, mine]
                    copies.append(remote(slot, slot, send_sem.at[batch, step], recv_sem.at[parity, batch, step], to if along_y else my_y, my_x if along_y else to))
                return copies

            def layer_out(layer):
                if layer == 0:
                    return a_ext, a_ud, 0, rx1a, rx2a
                if layer % 2:
                    return t_ext, t_ud, 1, rx1, rx2
                return h_ext, h_ud, 0, rx1, rx2

            def start_if(cond, copy):
                @pl.when(cond)
                def _():
                    copy.start()

            def send_columns(layer, sample):
                ext, _, parity, _, _ = layer_out(layer)
                for leaves, _, copy in column_copies(ext, parity, sample):
                    start_if(leaves, copy)

            def send_sums(layer, batch):
                _, _, parity, sums_one, _ = layer_out(layer)
                for copy in peers(sums_one, st1_send, st1_recv, parity, batch, True):
                    copy.start()

            def pass_on(layer, batch):
                ext, ud, parity, sums_one, sums_two = layer_out(layer)
                for index in range(BATCH):
                    for _, arrives, copy in column_copies(ext, parity, batch * BATCH + index):
                        @pl.when(arrives)
                        def _(copy=copy):
                            copy.wait_recv()
                for leaves, _, copy in row_copies(ext, ud, parity, batch):
                    start_if(leaves, copy)
                for copy in peers(sums_one, st1_send, st1_recv, parity, batch, True):
                    copy.wait_recv()
                total = sums_one[parity, batch, 0]
                for index in range(1, rows_n):
                    total = total + sums_one[parity, batch, index]
                parts = 2 if layer == 0 else 1
                for index in range(BATCH):
                    sums_two[parity, batch, my_x, index] = pack_groups(total[index], parts)

            def send_totals(layer, batch):
                _, _, parity, _, sums_two = layer_out(layer)
                for copy in peers(sums_two, st2_send, st2_recv, parity, batch, False):
                    copy.start()

            def boundary(layer, batch):
                @pl.when(batch > 0)
                def _():
                    send_sums(layer, batch - 1)

                @pl.when(batch >= 2)
                def _():
                    pass_on(layer, batch - 2)

                if layer > 0:
                    @pl.when(batch < 2)
                    def _():
                        pass_on(layer - 1, batches + batch - 2)

            def within(layer, batch, index):
                @pl.when((index == 1) & (batch >= 2))
                def _():
                    send_totals(layer, batch - 2)

                if layer > 0:
                    @pl.when((index == 1) & (batch < 2))
                    def _():
                        send_totals(layer - 1, batches + batch - 2)

            def await_batch(layer, batch):
                ext, ud, parity, sums_one, sums_two = layer_out(layer)
                rows = row_copies(ext, ud, parity, batch)
                for _, arrives, copy in rows:
                    @pl.when(arrives)
                    def _(copy=copy):
                        copy.wait_recv()
                for leaves, _, copy in rows:
                    @pl.when(leaves)
                    def _(copy=copy):
                        copy.wait_send()
                for index in range(BATCH):
                    for leaves, _, copy in column_copies(ext, parity, batch * BATCH + index):
                        @pl.when(leaves)
                        def _(copy=copy):
                            copy.wait_send()
                for copy in peers(sums_one, st1_send, st1_recv, parity, batch, True):
                    copy.wait_send()
                for copy in peers(sums_two, st2_send, st2_recv, parity, batch, False):
                    copy.wait()

            def group_total(value, per_group):
                lane = lax.broadcasted_iota(jnp.int32, value.shape, 1)
                step = 1
                while step < per_group:
                    ahead = pltpu.roll(value, 128 - step, axis=1)
                    behind = pltpu.roll(value, step, axis=1)
                    value = value + jnp.where(lax.rem(lane, 2 * step) < step, ahead, behind)
                    step *= 2
                return value

            def pack_groups(sums, parts):
                rows = 2 * parts
                groups = group_total(sums, 128 * parts // GROUPS)
                lane = lax.rem(lax.broadcasted_iota(jnp.int32, (1, 128), 1), rows)
                packed = groups[0:1]
                for row in range(1, rows):
                    packed = jnp.where(lane == row, groups[row:row + 1], packed)
                return packed

            def unpack_groups(packed, parts):
                rows = 2 * parts
                lane = lax.rem(lax.broadcasted_iota(jnp.int32, (1, 128), 1), rows)
                return [group_total(jnp.where(lane == row, packed, 0.0), rows) for row in range(rows)]

            def scale_shift(layer, sample):
                _, _, parity, _, sums_two = layer_out(layer)
                batch, index = sample // BATCH, lax.rem(sample, BATCH)
                total = sums_two[parity, batch, 0, index]
                for source in range(1, cols_n):
                    total = total + sums_two[parity, batch, source, index]
                parts = 2 if layer == 0 else 1
                moments = unpack_groups(total * (1.0 / (pixel_count * (128 * parts // GROUPS))), parts)
                pair = (norm_first[...] if layer == 0 else norm_rest[layer - 1]).astype(f32)
                result = []
                for part in range(parts):
                    mean, square = moments[part], moments[parts + part]
                    inv = lax.rsqrt(square - mean * mean + GN_EPS)
                    scale = inv * pair[0:1, part * 128:(part + 1) * 128]
                    shift = pair[1:2, part * 128:(part + 1) * 128] - mean * scale
                    result.append((0.5 * scale, 0.5 * shift))
                if parts == 1:
                    return result[0]
                return tuple(jnp.concatenate([result[0][i], result[1][i]], axis=1) for i in range(2))

            half_planes = planes // 2

            def activate(layer, sample):
                ext, ud, _, _, _ = layer_out(layer)
                upper, lower = (act_a0, act_a1) if layer == 0 else (act_m0, act_m1)
                chans = 256 if layer == 0 else 128
                scale, shift = scale_shift(layer, sample)
                scale3 = scale.reshape(1, 1, chans)
                shift3 = shift.reshape(1, 1, chans)
                shape = (ext_w, lanes, chans)
                col_id = lax.broadcasted_iota(jnp.int32, shape, 0)
                row_id = lax.broadcasted_iota(jnp.int32, shape, 1)
                in_cols = (col_id >= jnp.where(has_left, 0, 1)) & (col_id <= jnp.where(has_right, ext_w - 1, ext_w - 2))

                def silu(x):
                    half = x.astype(f32) * scale3 + shift3
                    return half + half * jnp.tanh(half)

                def put(plane, cols, value):
                    if plane <= half_planes + 1:
                        upper[plane // 2, plane % 2, cols] = value
                    if plane >= half_planes:
                        lower[(plane - half_planes) // 2, plane % 2, cols] = value

                def tile_plane(q):
                    put(q + 1, pl.ds(1, tile_w), silu(ext[sample, q, pl.ds(1, tile_w)]).astype(bf16))
                    for col, cond in ((0, has_left), (ext_w - 1, has_right)):
                        put(q + 1, pl.ds(col, 1), jnp.where(cond, silu(ext[sample, q, pl.ds(col, 1)]), 0.0).astype(bf16))

                def border_plane(near, plane, side, cond, turn, edge):
                    own = pltpu.roll(jnp.where(in_cols, silu(ext[sample, near]), 0.0), turn, axis=1)
                    other = pltpu.roll(jnp.where(in_cols & cond, silu(ud[side, sample]), 0.0), turn, axis=1)
                    put(plane, slice(None), jnp.where(row_id == edge, other, own).astype(bf16))

                def fill_upper():
                    border_plane(planes - 1, 0, 0, has_up, 1, 0)
                    for q in range(half_planes + 1):
                        tile_plane(q)

                def fill_lower():
                    for q in range(half_planes + 1, planes):
                        tile_plane(q)
                    border_plane(0, planes + 1, 1, has_down, lanes - 1, lanes - 1)

                return fill_upper, fill_lower

            def activate_convolve(layer, sample):
                fill_upper, fill_lower = activate(layer - 1, sample)
                chans = 256 if layer == 1 else 128
                ext, _, parity, sums_one, _ = layer_out(layer)
                bias_rows = bias_rest[...].astype(f32)
                bias = bias_rows[layer - 1:layer]
                if layer == 2:
                    bias = bias + bias_rows[6:7]
                weights = wp_first if layer == 1 else wp_rest.at[layer - 2]
                sums = [jnp.zeros((8, 128), f32), jnp.zeros((8, 128), f32)]
                parts = 4
                share = pairs // parts

                def product(part):
                    src = ((act_a0, act_a1) if layer == 1 else (act_m0, act_m1))[part // 2]
                    base = part % 2 * share
                    pieces = [src[pl.ds(base + j // 2, share), j % 2, pl.ds(dc, tile_w)].reshape(share * tile_w * lanes, chans) for dc in range(3) for j in range(4)]
                    return jnp.dot(jnp.concatenate(pieces, axis=1), weights[...], preferred_element_type=f32)

                def finish(part, accum):
                    for k in range(share):
                        for odd in range(2):
                            q = 2 * (part * share + k) + odd
                            value = accum[k * 128:(k + 1) * 128, odd * 128:(odd + 1) * 128].reshape(tile_w, lanes, 128) + bias.reshape(1, 1, 128)
                            if layer == 2:
                                skip = jnp.dot(a_ext[sample, q, pl.ds(1, tile_w)].reshape(128, 256), w_short[...], preferred_element_type=f32)
                                value = value + skip.reshape(tile_w, lanes, 128)
                            elif layer % 2 == 0:
                                value = value + ext[sample, q, pl.ds(1, tile_w)].astype(f32)
                            value = value.astype(bf16)
                            ext[sample, q, pl.ds(1, tile_w)] = value
                            wide = value.astype(f32).reshape(tile_w * 2, 8, 128)
                            sums[0] = sums[0] + jnp.sum(wide, axis=0)
                            sums[1] = sums[1] + jnp.sum(wide * wide, axis=0)

                fill_upper()
                first = [product(0), product(1)]
                fill_lower()
                for part in range(2):
                    finish(part, first[part])
                second = [product(2), product(3)]
                for part in range(2):
                    finish(2 + part, second[part])
                sums_one[parity, sample // BATCH, my_y, lax.rem(sample, BATCH)] = jnp.concatenate(
                    [jnp.sum(sums[0], axis=0, keepdims=True), jnp.sum(sums[1], axis=0, keepdims=True)], axis=0)

            def load_step(index, batch):
                sample = batch * BATCH + index
                slot = lax.rem(sample, 2)

                @pl.when(sample > 0)
                def _():
                    send_columns(0, sample - 1)

                @pl.when(sample + 1 < samples)
                def _():
                    fetch(sample + 1, 1 - slot).start()

                within(0, batch, index)
                fetch(sample, slot).wait()
                for chunk in range(tile_h // 16):
                    piece = raw[slot, pl.ds(chunk * 16, 16)].astype(f32).reshape(16 * tile_w, 256)
                    stage_lo[pl.ds(chunk * 16 * tile_w, 16 * tile_w), :] = piece[:, :128]
                    stage_hi[pl.ds(chunk * 16 * tile_w, 16 * tile_w), :] = piece[:, 128:]
                for half, stage in ((0, stage_lo), (1, stage_hi)):
                    sum_one = jnp.zeros((lanes, 128), f32)
                    sum_two = jnp.zeros((lanes, 128), f32)
                    for q in range(planes):
                        for c in range(tile_w):
                            value = stage[pl.ds(q * tile_w + c, lanes, stride=planes * tile_w), :]
                            a_ext[sample, q, c + 1, :, half * 128:(half + 1) * 128] = value.astype(bf16)
                            sum_one = sum_one + value
                            sum_two = sum_two + value * value
                    rx1a[0, sample // BATCH, my_y, lax.rem(sample, BATCH), half:half + 1] = jnp.sum(sum_one, axis=0, keepdims=True)
                    rx1a[0, sample // BATCH, my_y, lax.rem(sample, BATCH), half + 2:half + 3] = jnp.sum(sum_two, axis=0, keepdims=True)
                return batch

            def load_batch(batch, carry):
                boundary(0, batch)
                lax.fori_loop(0, BATCH, load_step, batch)
                return carry

            lax.fori_loop(0, batches, load_batch, 0)
            send_columns(0, samples - 1)
            send_sums(0, batches - 1)

            first_in.wait()
            rest_in.wait()
            pair_weights(wp_first, lambda dr, dc: w_first[dr, dc], 256)

            def pair_rest(index, carry):
                pair_weights(wp_rest.at[index], lambda dr, dc: w_rest[index, dr, dc], 128)
                return carry

            lax.fori_loop(0, 5, pair_rest, 0)

            for tap in range(9):
                taps3 = w_out[tap // 3, tap % 3].astype(f32)
                w_head[pl.ds(8 * tap, 8), :] = jnp.concatenate([taps3, jnp.zeros((5, 128), f32)], axis=0)
            from_id = lax.broadcasted_iota(jnp.int32, (tile_h, tile_h), 0)
            to_id = lax.broadcasted_iota(jnp.int32, (tile_h, tile_h), 1)
            reorder[...] = jnp.where(lax.rem(from_id, lanes) * planes + from_id // lanes == to_id, 1.0, 0.0).astype(bf16)

            for layer in range(1, 7):
                def conv_step(index, batch, layer=layer):
                    sample = batch * BATCH + index

                    @pl.when(sample > 0)
                    def _():
                        send_columns(layer, sample - 1)

                    within(layer, batch, index)
                    activate_convolve(layer, sample)
                    return batch

                def conv_batch(batch, carry, layer=layer, conv_step=conv_step):
                    boundary(layer, batch)
                    await_batch(layer - 1, batch)
                    lax.fori_loop(0, BATCH, conv_step, batch)
                    return carry

                lax.fori_loop(0, batches, conv_batch, 0)
                send_columns(layer, samples - 1)
                send_sums(layer, batches - 1)

            def head_step(index, batch):
                sample = batch * BATCH + index

                @pl.when((index == 1) & (batch < 2))
                def _():
                    send_totals(6, batches + batch - 2)

                for fill in activate(6, sample):
                    fill()
                rows = half_planes + 2
                flat = jnp.concatenate([act_m0[...].reshape(rows, ext_w, lanes, 128), act_m1[...].reshape(rows, ext_w, lanes, 128)[2:]], axis=0)
                flat = jnp.swapaxes(flat, 0, 1).reshape(ext_w * column_lanes, 128)
                flat = jnp.concatenate([flat, jnp.zeros((flat_width - flat.shape[0], 128), bf16)], axis=0)
                taps = lax.dot_general(w_head[...].astype(bf16), flat, (((1,), (1,)), ((), ())), preferred_element_type=f32)
                image = taps[0:8]
                for tap in range(1, 9):
                    offset = (tap % 3) * column_lanes + (tap // 3) * lanes
                    image = image + pltpu.roll(taps[8 * tap:8 * tap + 8], flat_width - offset, axis=1)
                rest = jnp.concatenate([image[:, c * column_lanes:c * column_lanes + tile_h] for c in range(tile_w)], axis=0)
                moved = jnp.zeros(rest.shape, f32)
                for _ in range(3):
                    piece = rest.astype(bf16)
                    moved = moved + jnp.dot(piece, reorder[...], preferred_element_type=f32)
                    rest = rest - piece.astype(f32)
                for side in range(tile_h // 128):
                    image_rows[side] = moved[:, side * 128:(side + 1) * 128]
                for chan in range(3):
                    for side in range(tile_h // 128):
                        out_ref[sample, chan, :, side * 128:(side + 1) * 128] = image_rows[side, pl.ds(chan, tile_w, stride=8), :] + bias_out[chan]
                return batch

            def head_batch(batch, carry):
                @pl.when(batch < 2)
                def _():
                    pass_on(6, batches + batch - 2)

                await_batch(6, batch)
                lax.fori_loop(0, BATCH, head_step, batch)
                return carry

            lax.fori_loop(0, batches, head_batch, 0)

        return kernel, lanes, planes, ext_w

    def local_decode(act_in, norm_first, w_first, w_short, norm_rest, w_rest, bias_rest, w_out, bias_out):
        samples, tile_h, tile_w, _ = act_in.shape
        kernel, lanes, planes, ext_w = make_kernel(samples, tile_h, tile_w)
        batches = samples // BATCH
        vmem = pl.BlockSpec(memory_space=pltpu.VMEM)
        hbm = pl.BlockSpec(memory_space=pl.ANY)
        scratch = [
            pltpu.VMEM((samples, planes, ext_w, lanes, 256), bf16),
            pltpu.VMEM((samples, planes, ext_w, lanes, 128), bf16),
            pltpu.VMEM((samples, planes, ext_w, lanes, 128), bf16),
            pltpu.VMEM((2, samples, ext_w, lanes, 256), bf16),
            pltpu.VMEM((2, samples, ext_w, lanes, 128), bf16),
            pltpu.VMEM((2, samples, ext_w, lanes, 128), bf16),
            pltpu.VMEM((planes // 4 + 1, 2, ext_w, lanes, 256), bf16),
            pltpu.VMEM((planes // 4 + 1, 2, ext_w, lanes, 256), bf16),
            pltpu.VMEM((planes // 4 + 1, 2, ext_w, lanes, 128), bf16),
            pltpu.VMEM((planes // 4 + 1, 2, ext_w, lanes, 128), bf16),
            pltpu.VMEM((3, 3, 256, 128), bf16),
            pltpu.VMEM((5, 3, 3, 128, 128), bf16),
            pltpu.VMEM((12 * 256, 256), bf16),
            pltpu.VMEM((5, 12 * 128, 256), bf16),
            pltpu.VMEM((72, 128), f32),
            pltpu.VMEM((tile_h, tile_h), bf16),
            pltpu.VMEM((tile_h // 128, 8 * tile_w, 128), f32),
            pltpu.VMEM((2, tile_h, tile_w, 256), bf16),
            pltpu.VMEM((tile_h * tile_w, 128), f32),
            pltpu.VMEM((tile_h * tile_w, 128), f32),
            pltpu.VMEM((2, batches, rows_n, BATCH, 2, 128), f32),
            pltpu.VMEM((2, batches, cols_n, BATCH, 1, 128), f32),
            pltpu.VMEM((1, batches, rows_n, BATCH, 4, 128), f32),
            pltpu.VMEM((1, batches, cols_n, BATCH, 1, 128), f32),
            pltpu.SemaphoreType.DMA((2,)),
            pltpu.SemaphoreType.DMA((2,)),
            pltpu.SemaphoreType.DMA((samples, 2)),
            pltpu.SemaphoreType.DMA((2, samples, 2)),
            pltpu.SemaphoreType.DMA((batches, 2)),
            pltpu.SemaphoreType.DMA((2, batches, 2)),
            pltpu.SemaphoreType.DMA((batches, rows_n)),
            pltpu.SemaphoreType.DMA((2, batches, rows_n)),
            pltpu.SemaphoreType.DMA((batches, cols_n)),
            pltpu.SemaphoreType.DMA((2, batches, cols_n)),
        ]
        image = pl.pallas_call(
            kernel,
            out_shape=jax.ShapeDtypeStruct((samples, 3, tile_w, tile_h), f32),
            in_specs=[hbm, vmem, vmem, vmem, pl.BlockSpec(memory_space=pltpu.SMEM), hbm, vmem, hbm, vmem],
            out_specs=vmem,
            scratch_shapes=scratch,
            compiler_params=pltpu.CompilerParams(collective_id=0, has_side_effects=True, vmem_limit_bytes=60 * 1024 * 1024),
        )(act_in, norm_first, norm_rest, bias_rest, bias_out.astype(f32), w_first, w_short, w_rest, w_out.transpose(0, 1, 3, 2))
        return image.transpose(0, 3, 2, 1)

    return jax.shard_map(local_decode, mesh=mesh, in_specs=(tile_spec, replicated, replicated, replicated, replicated, replicated, replicated, replicated, replicated), out_specs=tile_spec, check_vma=False)
```

```python
import jax
import jax.numpy as jnp
from jax import lax
from jax.experimental import pallas as pl
from jax.experimental.pallas import tpu as pltpu
from jax.sharding import PartitionSpec as P

GROUPS = 32
GN_EPS = 1e-6
MESH = pl.DeviceIdType.MESH
BATCH = 3


def solution(mesh):
    rows_n = mesh.shape["sy"]
    cols_n = mesh.shape["sx"]
    tile_spec = P("dp", "sy", "sx", None)
    replicated = P()
    bf16 = jnp.bfloat16
    f32 = jnp.float32

    def make_kernel(samples, tile_h, tile_w):
        lanes = 16
        planes = tile_h // lanes
        ext_w = tile_w + 2
        pairs = planes // 2
        pixel_count = float(tile_h * rows_n * tile_w * cols_n)

        batches = samples // BATCH
        column_lanes = (planes + 2) * lanes
        flat_width = -(-(ext_w * column_lanes) // 128) * 128

        def kernel(act_hbm, norm_first, norm_rest, bias_rest, bias_out, w_first_hbm, w_short, w_rest_hbm, w_out, out_ref,
                   a_ext, t_ext, h_ext, a_ud, t_ud, h_ud, act_a0, act_a1, act_m0, act_m1, w_first, w_rest, wp_first, wp_rest, w_head, reorder, image_rows,
                   raw, rx1, rx2, rx1a, rx2a,
                   raw_sem, weight_sem, first_send, first_recv, col_send, col_recv, row_send, row_recv, st1_send, st1_recv, st2_send, st2_recv):
            my_y = lax.axis_index("sy")
            my_x = lax.axis_index("sx")
            has_up = my_y > 0
            has_down = my_y < rows_n - 1
            has_left = my_x > 0
            has_right = my_x < cols_n - 1

            barrier = pltpu.get_barrier_semaphore()
            for step in range(1, rows_n * cols_n):
                other = lax.rem(my_y * cols_n + my_x + step, rows_n * cols_n)
                pl.semaphore_signal(barrier, inc=1, device_id={"sy": other // cols_n, "sx": lax.rem(other, cols_n)}, device_id_type=MESH)

            def fetch(sample):
                slot = lax.rem(sample, 2)
                return [pltpu.make_async_copy(act_hbm.at[sample, pl.ds(4 * part, 4)], raw.at[slot, pl.ds(4 * part, 4)], raw_sem.at[slot, part]) for part in range(lanes // 4)]

            first_in = pltpu.make_async_copy(w_first_hbm, w_first, weight_sem.at[0])
            rest_in = pltpu.make_async_copy(w_rest_hbm, w_rest, weight_sem.at[1])
            for copy in fetch(0):
                copy.start()
            first_in.start()
            rest_in.start()
            pl.semaphore_wait(barrier, rows_n * cols_n - 1)

            def pair_weights(dst, src, chans):
                for dc in range(3):
                    for j in range(4):
                        base = (dc * 4 + j) * chans
                        zero = jnp.zeros((chans, 128), bf16)
                        dst[pl.ds(base, chans), 0:128] = src(j, dc) if j < 3 else zero
                        dst[pl.ds(base, chans), 128:256] = src(j - 1, dc) if j > 0 else zero

            def span(batch):
                return pl.ds(batch * BATCH, BATCH)

            def remote(src, dst, send_sem, recv_sem, to_y, to_x):
                return pltpu.make_async_remote_copy(src_ref=src, dst_ref=dst, send_sem=send_sem, recv_sem=recv_sem,
                                                    device_id={"sy": to_y, "sx": to_x}, device_id_type=MESH)

            def column_copies(layer, batch):
                ext, _, parity, _, _ = layer_out(layer)
                moves = [(has_left, has_right, 1, ext_w - 1, my_x - 1), (has_right, has_left, ext_w - 2, 0, my_x + 1)]
                if layer == 0:
                    return [copy for index in range(BATCH) for copy in first_columns(batch * BATCH + index)]
                return [(leaves, arrives, remote(ext.at[span(batch), :, src], ext.at[span(batch), :, dst], col_send.at[batch, index], col_recv.at[parity, batch, index], my_y, to_x))
                        for index, (leaves, arrives, src, dst, to_x) in enumerate(moves)]

            def first_columns(sample):
                moves = [(has_left, has_right, 1, ext_w - 1, my_x - 1), (has_right, has_left, ext_w - 2, 0, my_x + 1)]
                return [(leaves, arrives, remote(a_ext.at[sample, :, src], a_ext.at[sample, :, dst], first_send.at[sample, index], first_recv.at[sample, index], my_y, to_x))
                        for index, (leaves, arrives, src, dst, to_x) in enumerate(moves)]

            def row_copies(ext, ud, parity, batch):
                moves = [(has_up, has_down, 0, 1, my_y - 1), (has_down, has_up, planes - 1, 0, my_y + 1)]
                return [(leaves, arrives, remote(ext.at[span(batch), src], ud.at[side, span(batch)], row_send.at[batch, side], row_recv.at[parity, batch, side], to_y, my_x))
                        for leaves, arrives, src, side, to_y in moves]

            def peers(buf, send_sem, recv_sem, parity, batch, along_y):
                mine = my_y if along_y else my_x
                count = rows_n if along_y else cols_n
                copies = []
                for step in range(1, count):
                    to = lax.rem(mine + step, count)
                    slot = buf.at[parity, batch, mine]
                    copies.append(remote(slot, slot, send_sem.at[batch, step], recv_sem.at[parity, batch, step], to if along_y else my_y, my_x if along_y else to))
                return copies

            def layer_out(layer):
                if layer == 0:
                    return a_ext, a_ud, 0, rx1a, rx2a
                if layer % 2:
                    return t_ext, t_ud, 1, rx1, rx2
                return h_ext, h_ud, 0, rx1, rx2

            def start_if(cond, copy):
                @pl.when(cond)
                def _():
                    copy.start()

            def send_batch(layer, batch):
                if layer > 0:
                    for leaves, _, copy in column_copies(layer, batch):
                        start_if(leaves, copy)
                send_sums(layer, batch)

            def send_sums(layer, batch):
                _, _, parity, sums_one, _ = layer_out(layer)
                for copy in peers(sums_one, st1_send, st1_recv, parity, batch, True):
                    copy.start()

            def pass_on(layer, batch):
                ext, ud, parity, sums_one, sums_two = layer_out(layer)
                for _, arrives, copy in column_copies(layer, batch):
                    @pl.when(arrives)
                    def _(copy=copy):
                        copy.wait_recv()
                for leaves, _, copy in row_copies(ext, ud, parity, batch):
                    start_if(leaves, copy)
                for copy in peers(sums_one, st1_send, st1_recv, parity, batch, True):
                    copy.wait_recv()
                total = sums_one[parity, batch, 0]
                for index in range(1, rows_n):
                    total = total + sums_one[parity, batch, index]
                parts = 2 if layer == 0 else 1
                for index in range(BATCH):
                    sums_two[parity, batch, my_x, index] = pack_groups(total[index], parts)

            def send_totals(layer, batch):
                _, _, parity, _, sums_two = layer_out(layer)
                for copy in peers(sums_two, st2_send, st2_recv, parity, batch, False):
                    copy.start()

            def boundary(layer, batch):
                if layer < 7:
                    @pl.when(batch > 0)
                    def _():
                        send_batch(layer, batch - 1)

                    @pl.when(batch >= 3)
                    def _():
                        send_totals(layer, batch - 3)

                if layer > 0:
                    @pl.when(batch < 3)
                    def _():
                        send_totals(layer - 1, batches + batch - 3)

                if layer < 7:
                    @pl.when(batch >= 2)
                    def _():
                        pass_on(layer, batch - 2)

                if layer > 0:
                    @pl.when(batch < 2)
                    def _():
                        pass_on(layer - 1, batches + batch - 2)

            def await_batch(layer, batch):
                ext, ud, parity, sums_one, sums_two = layer_out(layer)
                rows = row_copies(ext, ud, parity, batch)
                for _, arrives, copy in rows:
                    @pl.when(arrives)
                    def _(copy=copy):
                        copy.wait_recv()
                for leaves, _, copy in rows:
                    @pl.when(leaves)
                    def _(copy=copy):
                        copy.wait_send()
                for leaves, _, copy in column_copies(layer, batch):
                    @pl.when(leaves)
                    def _(copy=copy):
                        copy.wait_send()
                for copy in peers(sums_one, st1_send, st1_recv, parity, batch, True):
                    copy.wait_send()
                for copy in peers(sums_two, st2_send, st2_recv, parity, batch, False):
                    copy.wait()

            def group_total(value, per_group):
                lane = lax.broadcasted_iota(jnp.int32, value.shape, 1)
                step = 1
                while step < per_group:
                    ahead = pltpu.roll(value, 128 - step, axis=1)
                    behind = pltpu.roll(value, step, axis=1)
                    value = value + jnp.where(lax.rem(lane, 2 * step) < step, ahead, behind)
                    step *= 2
                return value

            def pack_groups(sums, parts):
                rows = 2 * parts
                groups = group_total(sums, 128 * parts // GROUPS)
                lane = lax.rem(lax.broadcasted_iota(jnp.int32, (1, 128), 1), rows)
                packed = groups[0:1]
                for row in range(1, rows):
                    packed = jnp.where(lane == row, groups[row:row + 1], packed)
                return packed

            def unpack_groups(packed, parts):
                rows = 2 * parts
                lane = lax.rem(lax.broadcasted_iota(jnp.int32, (1, 128), 1), rows)
                return [group_total(jnp.where(lane == row, packed, 0.0), rows) for row in range(rows)]

            def scale_shift(layer, sample):
                _, _, parity, _, sums_two = layer_out(layer)
                batch, index = sample // BATCH, lax.rem(sample, BATCH)
                total = sums_two[parity, batch, 0, index]
                for source in range(1, cols_n):
                    total = total + sums_two[parity, batch, source, index]
                parts = 2 if layer == 0 else 1
                moments = unpack_groups(total * (1.0 / (pixel_count * (128 * parts // GROUPS))), parts)
                pair = (norm_first[...] if layer == 0 else norm_rest[layer - 1]).astype(f32)
                result = []
                for part in range(parts):
                    mean, square = moments[part], moments[parts + part]
                    inv = lax.rsqrt(square - mean * mean + GN_EPS)
                    scale = inv * pair[0:1, part * 128:(part + 1) * 128]
                    shift = pair[1:2, part * 128:(part + 1) * 128] - mean * scale
                    result.append((0.5 * scale, 0.5 * shift))
                if parts == 1:
                    return result[0]
                return tuple(jnp.concatenate([result[0][i], result[1][i]], axis=1) for i in range(2))

            half_planes = planes // 2

            def activate(layer, sample):
                ext, ud, _, _, _ = layer_out(layer)
                upper, lower = (act_a0, act_a1) if layer == 0 else (act_m0, act_m1)
                chans = 256 if layer == 0 else 128
                scale, shift = scale_shift(layer, sample)
                scale3 = scale.reshape(1, 1, chans)
                shift3 = shift.reshape(1, 1, chans)
                shape = (ext_w, lanes, chans)
                col_id = lax.broadcasted_iota(jnp.int32, shape, 0)
                row_id = lax.broadcasted_iota(jnp.int32, shape, 1)
                in_cols = (col_id >= jnp.where(has_left, 0, 1)) & (col_id <= jnp.where(has_right, ext_w - 1, ext_w - 2))

                def silu(x):
                    half = x.astype(f32) * scale3 + shift3
                    return half + half * jnp.tanh(half)

                def put(plane, cols, value):
                    if plane <= half_planes + 1:
                        upper[plane // 2, plane % 2, cols] = value
                    if plane >= half_planes:
                        lower[(plane - half_planes) // 2, plane % 2, cols] = value

                def tile_plane(q):
                    put(q + 1, pl.ds(1, tile_w), silu(ext[sample, q, pl.ds(1, tile_w)]).astype(bf16))
                    for col, cond in ((0, has_left), (ext_w - 1, has_right)):
                        put(q + 1, pl.ds(col, 1), jnp.where(cond, silu(ext[sample, q, pl.ds(col, 1)]), 0.0).astype(bf16))

                def border_plane(near, plane, side, cond, turn, edge):
                    own = pltpu.roll(jnp.where(in_cols, silu(ext[sample, near]), 0.0), turn, axis=1)
                    other = pltpu.roll(jnp.where(in_cols & cond, silu(ud[side, sample]), 0.0), turn, axis=1)
                    put(plane, slice(None), jnp.where(row_id == edge, other, own).astype(bf16))

                def fill_upper():
                    border_plane(planes - 1, 0, 0, has_up, 1, 0)
                    for q in range(half_planes + 1):
                        tile_plane(q)

                def fill_lower():
                    for q in range(half_planes + 1, planes):
                        tile_plane(q)
                    border_plane(0, planes + 1, 1, has_down, lanes - 1, lanes - 1)

                return fill_upper, fill_lower

            def activate_convolve(layer, sample):
                fill_upper, fill_lower = activate(layer - 1, sample)
                chans = 256 if layer == 1 else 128
                ext, _, parity, sums_one, _ = layer_out(layer)
                bias_rows = bias_rest[...].astype(f32)
                bias = bias_rows[layer - 1:layer]
                if layer == 2:
                    bias = bias + bias_rows[6:7]
                weights = wp_first if layer == 1 else wp_rest.at[layer - 2]
                sums = [jnp.zeros((8, 128), f32), jnp.zeros((8, 128), f32)]
                parts = 4
                share = pairs // parts

                def product(part):
                    src = ((act_a0, act_a1) if layer == 1 else (act_m0, act_m1))[part // 2]
                    base = part % 2 * share
                    pieces = [src[pl.ds(base + j // 2, share), j % 2, pl.ds(dc, tile_w)].reshape(share * tile_w * lanes, chans) for dc in range(3) for j in range(4)]
                    return jnp.dot(jnp.concatenate(pieces, axis=1), weights[...], preferred_element_type=f32)

                def finish(part, accum):
                    for k in range(share):
                        for odd in range(2):
                            q = 2 * (part * share + k) + odd
                            value = accum[k * 128:(k + 1) * 128, odd * 128:(odd + 1) * 128].reshape(tile_w, lanes, 128) + bias.reshape(1, 1, 128)
                            if layer == 2:
                                skip = jnp.dot(a_ext[sample, q, pl.ds(1, tile_w)].reshape(128, 256), w_short[...], preferred_element_type=f32)
                                value = value + skip.reshape(tile_w, lanes, 128)
                            elif layer % 2 == 0:
                                value = value + ext[sample, q, pl.ds(1, tile_w)].astype(f32)
                            value = value.astype(bf16)
                            ext[sample, q, pl.ds(1, tile_w)] = value
                            wide = value.astype(f32).reshape(tile_w * 2, 8, 128)
                            sums[0] = sums[0] + jnp.sum(wide, axis=0)
                            sums[1] = sums[1] + jnp.sum(wide * wide, axis=0)

                fill_upper()
                first = [product(0), product(1)]
                fill_lower()
                for part in range(2):
                    finish(part, first[part])
                second = [product(2), product(3)]
                for part in range(2):
                    finish(2 + part, second[part])
                sums_one[parity, sample // BATCH, my_y, lax.rem(sample, BATCH)] = jnp.concatenate(
                    [jnp.sum(sums[0], axis=0, keepdims=True), jnp.sum(sums[1], axis=0, keepdims=True)], axis=0)

            def load_step(index, batch):
                sample = batch * BATCH + index

                @pl.when(sample > 0)
                def _():
                    for leaves, _, copy in first_columns(sample - 1):
                        start_if(leaves, copy)

                @pl.when(sample + 1 < samples)
                def _():
                    for copy in fetch(sample + 1):
                        copy.start()

                for copy in fetch(sample):
                    copy.wait()
                slot = lax.rem(sample, 2)
                sum_one = jnp.zeros((8, 256), f32)
                sum_two = jnp.zeros((8, 256), f32)
                for q in range(planes):
                    value = jnp.swapaxes(raw[slot, :, q].astype(f32), 0, 1)
                    a_ext[sample, q, pl.ds(1, tile_w)] = value.astype(bf16)
                    wide = value.reshape(2 * tile_w, 8, 256)
                    sum_one = sum_one + jnp.sum(wide, axis=0)
                    sum_two = sum_two + jnp.sum(wide * wide, axis=0)
                one = jnp.sum(sum_one, axis=0, keepdims=True)
                two = jnp.sum(sum_two, axis=0, keepdims=True)
                rx1a[0, batch, my_y, index] = jnp.concatenate([one[:, :128], one[:, 128:], two[:, :128], two[:, 128:]], axis=0)
                return batch

            def load_batch(batch, carry):
                boundary(0, batch)
                lax.fori_loop(0, BATCH, load_step, batch)
                return carry

            lax.fori_loop(0, batches, load_batch, 0)
            for leaves, _, copy in first_columns(samples - 1):
                start_if(leaves, copy)
            send_batch(0, batches - 1)

            first_in.wait()
            rest_in.wait()
            pair_weights(wp_first, lambda dr, dc: w_first[dr, dc], 256)

            def pair_rest(index, carry):
                pair_weights(wp_rest.at[index], lambda dr, dc: w_rest[index, dr, dc], 128)
                return carry

            lax.fori_loop(0, 5, pair_rest, 0)

            for tap in range(9):
                taps3 = w_out[tap // 3, tap % 3].astype(f32)
                w_head[pl.ds(8 * tap, 8), :] = jnp.concatenate([taps3, jnp.zeros((5, 128), f32)], axis=0)
            from_id = lax.broadcasted_iota(jnp.int32, (tile_h, tile_h), 0)
            to_id = lax.broadcasted_iota(jnp.int32, (tile_h, tile_h), 1)
            reorder[...] = jnp.where(lax.rem(from_id, lanes) * planes + from_id // lanes == to_id, 1.0, 0.0).astype(bf16)

            for layer in range(1, 7):
                def conv_step(index, batch, layer=layer):
                    activate_convolve(layer, batch * BATCH + index)
                    return batch

                def conv_batch(batch, carry, layer=layer, conv_step=conv_step):
                    boundary(layer, batch)
                    await_batch(layer - 1, batch)
                    lax.fori_loop(0, BATCH, conv_step, batch)
                    return carry

                lax.fori_loop(0, batches, conv_batch, 0)
                send_batch(layer, batches - 1)

            def head_step(index, batch):
                sample = batch * BATCH + index

                for fill in activate(6, sample):
                    fill()
                rows = half_planes + 2
                flat = jnp.concatenate([act_m0[...].reshape(rows, ext_w, lanes, 128), act_m1[...].reshape(rows, ext_w, lanes, 128)[2:]], axis=0)
                flat = jnp.swapaxes(flat, 0, 1).reshape(ext_w * column_lanes, 128)
                flat = jnp.concatenate([flat, jnp.zeros((flat_width - flat.shape[0], 128), bf16)], axis=0)
                taps = lax.dot_general(w_head[...].astype(bf16), flat, (((1,), (1,)), ((), ())), preferred_element_type=f32)
                image = taps[0:8]
                for tap in range(1, 9):
                    offset = (tap % 3) * column_lanes + (tap // 3) * lanes
                    image = image + pltpu.roll(taps[8 * tap:8 * tap + 8], flat_width - offset, axis=1)
                rest = jnp.concatenate([image[:, c * column_lanes:c * column_lanes + tile_h] for c in range(tile_w)], axis=0)
                moved = jnp.zeros(rest.shape, f32)
                for _ in range(3):
                    piece = rest.astype(bf16)
                    moved = moved + jnp.dot(piece, reorder[...], preferred_element_type=f32)
                    rest = rest - piece.astype(f32)
                for side in range(tile_h // 128):
                    image_rows[side] = moved[:, side * 128:(side + 1) * 128]
                for chan in range(3):
                    for side in range(tile_h // 128):
                        out_ref[sample, chan, :, side * 128:(side + 1) * 128] = image_rows[side, pl.ds(chan, tile_w, stride=8), :] + bias_out[chan]
                return batch

            def head_batch(batch, carry):
                boundary(7, batch)
                await_batch(6, batch)
                lax.fori_loop(0, BATCH, head_step, batch)
                return carry

            lax.fori_loop(0, batches, head_batch, 0)

        return kernel, lanes, planes, ext_w

    def local_decode(act_in, norm_first, w_first, w_short, norm_rest, w_rest, bias_rest, w_out, bias_out):
        samples, tile_h, tile_w, _ = act_in.shape
        kernel, lanes, planes, ext_w = make_kernel(samples, tile_h, tile_w)
        batches = samples // BATCH
        vmem = pl.BlockSpec(memory_space=pltpu.VMEM)
        hbm = pl.BlockSpec(memory_space=pl.ANY)
        scratch = [
            pltpu.VMEM((samples, planes, ext_w, lanes, 256), bf16),
            pltpu.VMEM((samples, planes, ext_w, lanes, 128), bf16),
            pltpu.VMEM((samples, planes, ext_w, lanes, 128), bf16),
            pltpu.VMEM((2, samples, ext_w, lanes, 256), bf16),
            pltpu.VMEM((2, samples, ext_w, lanes, 128), bf16),
            pltpu.VMEM((2, samples, ext_w, lanes, 128), bf16),
            pltpu.VMEM((planes // 4 + 1, 2, ext_w, lanes, 256), bf16),
            pltpu.VMEM((planes // 4 + 1, 2, ext_w, lanes, 256), bf16),
            pltpu.VMEM((planes // 4 + 1, 2, ext_w, lanes, 128), bf16),
            pltpu.VMEM((planes // 4 + 1, 2, ext_w, lanes, 128), bf16),
            pltpu.VMEM((3, 3, 256, 128), bf16),
            pltpu.VMEM((5, 3, 3, 128, 128), bf16),
            pltpu.VMEM((12 * 256, 256), bf16),
            pltpu.VMEM((5, 12 * 128, 256), bf16),
            pltpu.VMEM((72, 128), f32),
            pltpu.VMEM((tile_h, tile_h), bf16),
            pltpu.VMEM((tile_h // 128, 8 * tile_w, 128), f32),
            pltpu.VMEM((2, lanes, planes, tile_w, 256), bf16),
            pltpu.VMEM((2, batches, rows_n, BATCH, 2, 128), f32),
            pltpu.VMEM((2, batches, cols_n, BATCH, 1, 128), f32),
            pltpu.VMEM((1, batches, rows_n, BATCH, 4, 128), f32),
            pltpu.VMEM((1, batches, cols_n, BATCH, 1, 128), f32),
            pltpu.SemaphoreType.DMA((2, lanes // 4)),
            pltpu.SemaphoreType.DMA((2,)),
            pltpu.SemaphoreType.DMA((samples, 2)),
            pltpu.SemaphoreType.DMA((samples, 2)),
            pltpu.SemaphoreType.DMA((batches, 2)),
            pltpu.SemaphoreType.DMA((2, batches, 2)),
            pltpu.SemaphoreType.DMA((batches, 2)),
            pltpu.SemaphoreType.DMA((2, batches, 2)),
            pltpu.SemaphoreType.DMA((batches, rows_n)),
            pltpu.SemaphoreType.DMA((2, batches, rows_n)),
            pltpu.SemaphoreType.DMA((batches, cols_n)),
            pltpu.SemaphoreType.DMA((2, batches, cols_n)),
        ]
        image = pl.pallas_call(
            kernel,
            out_shape=jax.ShapeDtypeStruct((samples, 3, tile_w, tile_h), f32),
            in_specs=[hbm, vmem, vmem, vmem, pl.BlockSpec(memory_space=pltpu.SMEM), hbm, vmem, hbm, vmem],
            out_specs=vmem,
            scratch_shapes=scratch,
            compiler_params=pltpu.CompilerParams(collective_id=0, has_side_effects=True, vmem_limit_bytes=60 * 1024 * 1024),
        )(act_in.reshape(samples, lanes, planes, tile_w, 256), norm_first, norm_rest, bias_rest, bias_out.astype(f32), w_first, w_short, w_rest, w_out.transpose(0, 1, 3, 2))
        return image.transpose(0, 3, 2, 1)

    return jax.shard_map(local_decode, mesh=mesh, in_specs=(tile_spec, replicated, replicated, replicated, replicated, replicated, replicated, replicated, replicated), out_specs=tile_spec, check_vma=False)
```

```python
import jax
import jax.numpy as jnp
from jax import lax
from jax.experimental import pallas as pl
from jax.experimental.pallas import tpu as pltpu
from jax.sharding import PartitionSpec as P

GROUPS = 32
GN_EPS = 1e-6
MESH = pl.DeviceIdType.MESH
BATCH = 3


def solution(mesh):
    rows_n = mesh.shape["sy"]
    cols_n = mesh.shape["sx"]
    tile_spec = P("dp", "sy", "sx", None)
    replicated = P()
    bf16 = jnp.bfloat16
    f32 = jnp.float32

    def make_kernel(samples, tile_h, tile_w):
        lanes = 16
        planes = tile_h // lanes
        ext_w = tile_w + 2
        pairs = planes // 2
        pixel_count = float(tile_h * rows_n * tile_w * cols_n)

        batches = samples // BATCH
        column_lanes = (planes + 2) * lanes
        flat_width = -(-(ext_w * column_lanes) // 128) * 128

        def kernel(act_hbm, norm_first, norm_rest, bias_rest, bias_out, w_first_hbm, w_short, w_rest_hbm, w_out, out_ref,
                   a_ext, t_ext, h_ext, a_ud, t_ud, h_ud, act_a0, act_a1, act_m0, act_m1, w_first, w_rest, wp_first, wp_rest, w_head, reorder, image_rows,
                   raw, rx1, rx2, rx1a, rx2a,
                   raw_sem, weight_sem, col_send, col_recv, row_send, row_recv, st1_send, st1_recv, st2_send, st2_recv):
            my_y = lax.axis_index("sy")
            my_x = lax.axis_index("sx")
            has_up = my_y > 0
            has_down = my_y < rows_n - 1
            has_left = my_x > 0
            has_right = my_x < cols_n - 1

            barrier = pltpu.get_barrier_semaphore()
            for step in range(1, rows_n * cols_n):
                other = lax.rem(my_y * cols_n + my_x + step, rows_n * cols_n)
                pl.semaphore_signal(barrier, inc=1, device_id={"sy": other // cols_n, "sx": lax.rem(other, cols_n)}, device_id_type=MESH)

            def fetch(sample):
                slot = lax.rem(sample, 2)
                return [pltpu.make_async_copy(act_hbm.at[sample, pl.ds(4 * part, 4)], raw.at[slot, pl.ds(4 * part, 4)], raw_sem.at[slot, part]) for part in range(lanes // 4)]

            first_in = pltpu.make_async_copy(w_first_hbm, w_first, weight_sem.at[0])
            rest_in = pltpu.make_async_copy(w_rest_hbm, w_rest, weight_sem.at[1])
            for copy in fetch(0):
                copy.start()
            first_in.start()
            rest_in.start()
            pl.semaphore_wait(barrier, rows_n * cols_n - 1)

            def pair_weights(dst, src, chans):
                for dc in range(3):
                    for j in range(4):
                        base = (dc * 4 + j) * chans
                        zero = jnp.zeros((chans, 128), bf16)
                        dst[pl.ds(base, chans), 0:128] = src(j, dc) if j < 3 else zero
                        dst[pl.ds(base, chans), 128:256] = src(j - 1, dc) if j > 0 else zero

            def span(batch):
                return pl.ds(batch * BATCH, BATCH)

            def remote(src, dst, send_sem, recv_sem, to_y, to_x):
                return pltpu.make_async_remote_copy(src_ref=src, dst_ref=dst, send_sem=send_sem, recv_sem=recv_sem,
                                                    device_id={"sy": to_y, "sx": to_x}, device_id_type=MESH)

            def sample_columns(layer, sample):
                ext, _, parity, _, _ = layer_out(layer)
                moves = [(has_left, has_right, 1, ext_w - 1, my_x - 1), (has_right, has_left, ext_w - 2, 0, my_x + 1)]
                return [(leaves, arrives, remote(ext.at[sample, :, src], ext.at[sample, :, dst], col_send.at[sample, index], col_recv.at[parity, sample, index], my_y, to_x))
                        for index, (leaves, arrives, src, dst, to_x) in enumerate(moves)]

            def column_copies(layer, batch):
                return [copy for index in range(BATCH) for copy in sample_columns(layer, batch * BATCH + index)]

            def row_copies(ext, ud, parity, batch):
                moves = [(has_up, has_down, 0, 1, my_y - 1), (has_down, has_up, planes - 1, 0, my_y + 1)]
                return [(leaves, arrives, remote(ext.at[span(batch), src], ud.at[side, span(batch)], row_send.at[batch, side], row_recv.at[parity, batch, side], to_y, my_x))
                        for leaves, arrives, src, side, to_y in moves]

            def peers(buf, send_sem, recv_sem, parity, batch, along_y):
                mine = my_y if along_y else my_x
                count = rows_n if along_y else cols_n
                copies = []
                for step in range(1, count):
                    to = lax.rem(mine + step, count)
                    slot = buf.at[parity, batch, mine]
                    copies.append(remote(slot, slot, send_sem.at[batch, step], recv_sem.at[parity, batch, step], to if along_y else my_y, my_x if along_y else to))
                return copies

            def layer_out(layer):
                if layer == 0:
                    return a_ext, a_ud, 0, rx1a, rx2a
                if layer % 2:
                    return t_ext, t_ud, 1, rx1, rx2
                return h_ext, h_ud, 0, rx1, rx2

            def start_if(cond, copy):
                @pl.when(cond)
                def _():
                    copy.start()

            def send_batch(layer, batch):
                if layer > 0:
                    for leaves, _, copy in column_copies(layer, batch):
                        start_if(leaves, copy)
                send_sums(layer, batch)

            def send_sums(layer, batch):
                _, _, parity, sums_one, _ = layer_out(layer)
                for copy in peers(sums_one, st1_send, st1_recv, parity, batch, True):
                    copy.start()

            def relay_rows(layer, batch):
                ext, ud, parity, _, _ = layer_out(layer)
                for _, arrives, copy in column_copies(layer, batch):
                    @pl.when(arrives)
                    def _(copy=copy):
                        copy.wait_recv()
                for leaves, _, copy in row_copies(ext, ud, parity, batch):
                    start_if(leaves, copy)

            def fold_sums(layer, batch):
                _, _, parity, sums_one, sums_two = layer_out(layer)
                for copy in peers(sums_one, st1_send, st1_recv, parity, batch, True):
                    copy.wait_recv()
                total = sums_one[parity, batch, 0]
                for index in range(1, rows_n):
                    total = total + sums_one[parity, batch, index]
                parts = 2 if layer == 0 else 1
                for index in range(BATCH):
                    sums_two[parity, batch, my_x, index] = pack_groups(total[index], parts)

            def send_totals(layer, batch):
                _, _, parity, _, sums_two = layer_out(layer)
                for copy in peers(sums_two, st2_send, st2_recv, parity, batch, False):
                    copy.start()

            def boundary(layer, batch):
                if layer < 7:
                    @pl.when(batch > 0)
                    def _():
                        send_batch(layer, batch - 1)

                    @pl.when(batch >= 3)
                    def _():
                        send_totals(layer, batch - 3)
                        relay_rows(layer, batch - 3)

                if layer > 0:
                    @pl.when(batch < 3)
                    def _():
                        send_totals(layer - 1, batches + batch - 3)
                        relay_rows(layer - 1, batches + batch - 3)

                if layer < 7:
                    @pl.when(batch >= 2)
                    def _():
                        fold_sums(layer, batch - 2)

                if layer > 0:
                    @pl.when(batch < 2)
                    def _():
                        fold_sums(layer - 1, batches + batch - 2)

            def await_batch(layer, batch):
                ext, ud, parity, sums_one, sums_two = layer_out(layer)
                rows = row_copies(ext, ud, parity, batch)
                for _, arrives, copy in rows:
                    @pl.when(arrives)
                    def _(copy=copy):
                        copy.wait_recv()
                for leaves, _, copy in rows:
                    @pl.when(leaves)
                    def _(copy=copy):
                        copy.wait_send()
                for leaves, _, copy in column_copies(layer, batch):
                    @pl.when(leaves)
                    def _(copy=copy):
                        copy.wait_send()
                for copy in peers(sums_one, st1_send, st1_recv, parity, batch, True):
                    copy.wait_send()
                for copy in peers(sums_two, st2_send, st2_recv, parity, batch, False):
                    copy.wait()

            def group_total(value, per_group):
                lane = lax.broadcasted_iota(jnp.int32, value.shape, 1)
                step = 1
                while step < per_group:
                    ahead = pltpu.roll(value, 128 - step, axis=1)
                    behind = pltpu.roll(value, step, axis=1)
                    value = value + jnp.where(lax.rem(lane, 2 * step) < step, ahead, behind)
                    step *= 2
                return value

            def pack_groups(sums, parts):
                rows = 2 * parts
                groups = group_total(sums, 128 * parts // GROUPS)
                lane = lax.rem(lax.broadcasted_iota(jnp.int32, (1, 128), 1), rows)
                packed = groups[0:1]
                for row in range(1, rows):
                    packed = jnp.where(lane == row, groups[row:row + 1], packed)
                return packed

            def unpack_groups(packed, parts):
                rows = 2 * parts
                lane = lax.rem(lax.broadcasted_iota(jnp.int32, (1, 128), 1), rows)
                return [group_total(jnp.where(lane == row, packed, 0.0), rows) for row in range(rows)]

            def scale_shift(layer, sample):
                _, _, parity, _, sums_two = layer_out(layer)
                batch, index = sample // BATCH, lax.rem(sample, BATCH)
                total = sums_two[parity, batch, 0, index]
                for source in range(1, cols_n):
                    total = total + sums_two[parity, batch, source, index]
                parts = 2 if layer == 0 else 1
                moments = unpack_groups(total * (1.0 / (pixel_count * (128 * parts // GROUPS))), parts)
                pair = (norm_first[...] if layer == 0 else norm_rest[layer - 1]).astype(f32)
                result = []
                for part in range(parts):
                    mean, square = moments[part], moments[parts + part]
                    inv = lax.rsqrt(square - mean * mean + GN_EPS)
                    scale = inv * pair[0:1, part * 128:(part + 1) * 128]
                    shift = pair[1:2, part * 128:(part + 1) * 128] - mean * scale
                    result.append((0.5 * scale, 0.5 * shift))
                if parts == 1:
                    return result[0]
                return tuple(jnp.concatenate([result[0][i], result[1][i]], axis=1) for i in range(2))

            half_planes = planes // 2

            def activate(layer, sample):
                ext, ud, _, _, _ = layer_out(layer)
                upper, lower = (act_a0, act_a1) if layer == 0 else (act_m0, act_m1)
                chans = 256 if layer == 0 else 128
                scale, shift = scale_shift(layer, sample)
                scale3 = scale.reshape(1, 1, chans)
                shift3 = shift.reshape(1, 1, chans)
                shape = (ext_w, lanes, chans)
                col_id = lax.broadcasted_iota(jnp.int32, shape, 0)
                row_id = lax.broadcasted_iota(jnp.int32, shape, 1)
                in_cols = (col_id >= jnp.where(has_left, 0, 1)) & (col_id <= jnp.where(has_right, ext_w - 1, ext_w - 2))

                def silu(x):
                    half = x.astype(f32) * scale3 + shift3
                    return half + half * jnp.tanh(half)

                def put(plane, cols, value):
                    if plane <= half_planes + 1:
                        upper[plane // 2, plane % 2, cols] = value
                    if plane >= half_planes:
                        lower[(plane - half_planes) // 2, plane % 2, cols] = value

                def tile_plane(q):
                    put(q + 1, pl.ds(1, tile_w), silu(ext[sample, q, pl.ds(1, tile_w)]).astype(bf16))
                    for col, cond in ((0, has_left), (ext_w - 1, has_right)):
                        put(q + 1, pl.ds(col, 1), jnp.where(cond, silu(ext[sample, q, pl.ds(col, 1)]), 0.0).astype(bf16))

                def border_plane(near, plane, side, cond, turn, edge):
                    own = pltpu.roll(jnp.where(in_cols, silu(ext[sample, near]), 0.0), turn, axis=1)
                    other = pltpu.roll(jnp.where(in_cols & cond, silu(ud[side, sample]), 0.0), turn, axis=1)
                    put(plane, slice(None), jnp.where(row_id == edge, other, own).astype(bf16))

                def fill_upper():
                    border_plane(planes - 1, 0, 0, has_up, 1, 0)
                    for q in range(half_planes + 1):
                        tile_plane(q)

                def fill_lower():
                    for q in range(half_planes + 1, planes):
                        tile_plane(q)
                    border_plane(0, planes + 1, 1, has_down, lanes - 1, lanes - 1)

                return fill_upper, fill_lower

            def activate_convolve(layer, sample):
                fill_upper, fill_lower = activate(layer - 1, sample)
                chans = 256 if layer == 1 else 128
                ext, _, parity, sums_one, _ = layer_out(layer)
                bias_rows = bias_rest[...].astype(f32)
                bias = bias_rows[layer - 1:layer]
                if layer == 2:
                    bias = bias + bias_rows[6:7]
                weights = wp_first if layer == 1 else wp_rest.at[layer - 2]
                sums = [jnp.zeros((8, 128), f32), jnp.zeros((8, 128), f32)]
                parts = 4
                share = pairs // parts

                def product(part):
                    src = ((act_a0, act_a1) if layer == 1 else (act_m0, act_m1))[part // 2]
                    base = part % 2 * share
                    pieces = [src[pl.ds(base + j // 2, share), j % 2, pl.ds(dc, tile_w)].reshape(share * tile_w * lanes, chans) for dc in range(3) for j in range(4)]
                    return jnp.dot(jnp.concatenate(pieces, axis=1), weights[...], preferred_element_type=f32)

                def finish(part, accum):
                    for k in range(share):
                        for odd in range(2):
                            q = 2 * (part * share + k) + odd
                            value = accum[k * 128:(k + 1) * 128, odd * 128:(odd + 1) * 128].reshape(tile_w, lanes, 128) + bias.reshape(1, 1, 128)
                            if layer == 2:
                                skip = jnp.dot(a_ext[sample, q, pl.ds(1, tile_w)].reshape(128, 256), w_short[...], preferred_element_type=f32)
                                value = value + skip.reshape(tile_w, lanes, 128)
                            elif layer % 2 == 0:
                                value = value + ext[sample, q, pl.ds(1, tile_w)].astype(f32)
                            value = value.astype(bf16)
                            ext[sample, q, pl.ds(1, tile_w)] = value
                            wide = value.astype(f32).reshape(tile_w * 2, 8, 128)
                            sums[0] = sums[0] + jnp.sum(wide, axis=0)
                            sums[1] = sums[1] + jnp.sum(wide * wide, axis=0)

                fill_upper()
                first = [product(0), product(1)]
                fill_lower()
                for part in range(2):
                    finish(part, first[part])
                second = [product(2), product(3)]
                for part in range(2):
                    finish(2 + part, second[part])
                sums_one[parity, sample // BATCH, my_y, lax.rem(sample, BATCH)] = jnp.concatenate(
                    [jnp.sum(sums[0], axis=0, keepdims=True), jnp.sum(sums[1], axis=0, keepdims=True)], axis=0)

            def load_step(index, batch):
                sample = batch * BATCH + index

                @pl.when(sample > 0)
                def _():
                    for leaves, _, copy in sample_columns(0, sample - 1):
                        start_if(leaves, copy)

                @pl.when(sample + 1 < samples)
                def _():
                    for copy in fetch(sample + 1):
                        copy.start()

                for copy in fetch(sample):
                    copy.wait()
                slot = lax.rem(sample, 2)
                sum_one = jnp.zeros((8, 256), f32)
                sum_two = jnp.zeros((8, 256), f32)
                for q in range(planes):
                    value = jnp.swapaxes(raw[slot, :, q].astype(f32), 0, 1)
                    a_ext[sample, q, pl.ds(1, tile_w)] = value.astype(bf16)
                    wide = value.reshape(2 * tile_w, 8, 256)
                    sum_one = sum_one + jnp.sum(wide, axis=0)
                    sum_two = sum_two + jnp.sum(wide * wide, axis=0)
                one = jnp.sum(sum_one, axis=0, keepdims=True)
                two = jnp.sum(sum_two, axis=0, keepdims=True)
                rx1a[0, batch, my_y, index] = jnp.concatenate([one[:, :128], one[:, 128:], two[:, :128], two[:, 128:]], axis=0)
                return batch

            def load_batch(batch, carry):
                boundary(0, batch)
                lax.fori_loop(0, BATCH, load_step, batch)
                return carry

            lax.fori_loop(0, batches, load_batch, 0)
            for leaves, _, copy in sample_columns(0, samples - 1):
                start_if(leaves, copy)
            send_batch(0, batches - 1)

            first_in.wait()
            rest_in.wait()
            pair_weights(wp_first, lambda dr, dc: w_first[dr, dc], 256)

            def pair_rest(index, carry):
                pair_weights(wp_rest.at[index], lambda dr, dc: w_rest[index, dr, dc], 128)
                return carry

            lax.fori_loop(0, 5, pair_rest, 0)

            for tap in range(9):
                taps3 = w_out[tap // 3, tap % 3].astype(f32)
                w_head[pl.ds(8 * tap, 8), :] = jnp.concatenate([taps3, jnp.zeros((5, 128), f32)], axis=0)
            from_id = lax.broadcasted_iota(jnp.int32, (tile_h, tile_h), 0)
            to_id = lax.broadcasted_iota(jnp.int32, (tile_h, tile_h), 1)
            reorder[...] = jnp.where(lax.rem(from_id, lanes) * planes + from_id // lanes == to_id, 1.0, 0.0).astype(bf16)

            for layer in range(1, 7):
                def conv_step(index, batch, layer=layer):
                    activate_convolve(layer, batch * BATCH + index)
                    return batch

                def conv_batch(batch, carry, layer=layer, conv_step=conv_step):
                    boundary(layer, batch)
                    await_batch(layer - 1, batch)
                    lax.fori_loop(0, BATCH, conv_step, batch)
                    return carry

                lax.fori_loop(0, batches, conv_batch, 0)
                send_batch(layer, batches - 1)

            def head_step(index, batch):
                sample = batch * BATCH + index

                for fill in activate(6, sample):
                    fill()
                rows = half_planes + 2
                flat = jnp.concatenate([act_m0[...].reshape(rows, ext_w, lanes, 128), act_m1[...].reshape(rows, ext_w, lanes, 128)[2:]], axis=0)
                flat = jnp.swapaxes(flat, 0, 1).reshape(ext_w * column_lanes, 128)
                flat = jnp.concatenate([flat, jnp.zeros((flat_width - flat.shape[0], 128), bf16)], axis=0)
                taps = lax.dot_general(w_head[...].astype(bf16), flat, (((1,), (1,)), ((), ())), preferred_element_type=f32)
                image = taps[0:8]
                for tap in range(1, 9):
                    offset = (tap % 3) * column_lanes + (tap // 3) * lanes
                    image = image + pltpu.roll(taps[8 * tap:8 * tap + 8], flat_width - offset, axis=1)
                rest = jnp.concatenate([image[:, c * column_lanes:c * column_lanes + tile_h] for c in range(tile_w)], axis=0)
                moved = jnp.zeros(rest.shape, f32)
                for _ in range(3):
                    piece = rest.astype(bf16)
                    moved = moved + jnp.dot(piece, reorder[...], preferred_element_type=f32)
                    rest = rest - piece.astype(f32)
                for side in range(tile_h // 128):
                    image_rows[side] = moved[:, side * 128:(side + 1) * 128]
                for chan in range(3):
                    for side in range(tile_h // 128):
                        out_ref[sample, chan, :, side * 128:(side + 1) * 128] = image_rows[side, pl.ds(chan, tile_w, stride=8), :] + bias_out[chan]
                return batch

            def head_batch(batch, carry):
                boundary(7, batch)
                await_batch(6, batch)
                lax.fori_loop(0, BATCH, head_step, batch)
                return carry

            lax.fori_loop(0, batches, head_batch, 0)

        return kernel, lanes, planes, ext_w

    def local_decode(act_in, norm_first, w_first, w_short, norm_rest, w_rest, bias_rest, w_out, bias_out):
        samples, tile_h, tile_w, _ = act_in.shape
        kernel, lanes, planes, ext_w = make_kernel(samples, tile_h, tile_w)
        batches = samples // BATCH
        vmem = pl.BlockSpec(memory_space=pltpu.VMEM)
        hbm = pl.BlockSpec(memory_space=pl.ANY)
        scratch = [
            pltpu.VMEM((samples, planes, ext_w, lanes, 256), bf16),
            pltpu.VMEM((samples, planes, ext_w, lanes, 128), bf16),
            pltpu.VMEM((samples, planes, ext_w, lanes, 128), bf16),
            pltpu.VMEM((2, samples, ext_w, lanes, 256), bf16),
            pltpu.VMEM((2, samples, ext_w, lanes, 128), bf16),
            pltpu.VMEM((2, samples, ext_w, lanes, 128), bf16),
            pltpu.VMEM((planes // 4 + 1, 2, ext_w, lanes, 256), bf16),
            pltpu.VMEM((planes // 4 + 1, 2, ext_w, lanes, 256), bf16),
            pltpu.VMEM((planes // 4 + 1, 2, ext_w, lanes, 128), bf16),
            pltpu.VMEM((planes // 4 + 1, 2, ext_w, lanes, 128), bf16),
            pltpu.VMEM((3, 3, 256, 128), bf16),
            pltpu.VMEM((5, 3, 3, 128, 128), bf16),
            pltpu.VMEM((12 * 256, 256), bf16),
            pltpu.VMEM((5, 12 * 128, 256), bf16),
            pltpu.VMEM((72, 128), f32),
            pltpu.VMEM((tile_h, tile_h), bf16),
            pltpu.VMEM((tile_h // 128, 8 * tile_w, 128), f32),
            pltpu.VMEM((2, lanes, planes, tile_w, 256), bf16),
            pltpu.VMEM((2, batches, rows_n, BATCH, 2, 128), f32),
            pltpu.VMEM((2, batches, cols_n, BATCH, 1, 128), f32),
            pltpu.VMEM((1, batches, rows_n, BATCH, 4, 128), f32),
            pltpu.VMEM((1, batches, cols_n, BATCH, 1, 128), f32),
            pltpu.SemaphoreType.DMA((2, lanes // 4)),
            pltpu.SemaphoreType.DMA((2,)),
            pltpu.SemaphoreType.DMA((samples, 2)),
            pltpu.SemaphoreType.DMA((2, samples, 2)),
            pltpu.SemaphoreType.DMA((batches, 2)),
            pltpu.SemaphoreType.DMA((2, batches, 2)),
            pltpu.SemaphoreType.DMA((batches, rows_n)),
            pltpu.SemaphoreType.DMA((2, batches, rows_n)),
            pltpu.SemaphoreType.DMA((batches, cols_n)),
            pltpu.SemaphoreType.DMA((2, batches, cols_n)),
        ]
        image = pl.pallas_call(
            kernel,
            out_shape=jax.ShapeDtypeStruct((samples, 3, tile_w, tile_h), f32),
            in_specs=[hbm, vmem, vmem, vmem, pl.BlockSpec(memory_space=pltpu.SMEM), hbm, vmem, hbm, vmem],
            out_specs=vmem,
            scratch_shapes=scratch,
            compiler_params=pltpu.CompilerParams(collective_id=0, has_side_effects=True, vmem_limit_bytes=60 * 1024 * 1024),
        )(act_in.reshape(samples, lanes, planes, tile_w, 256), norm_first, norm_rest, bias_rest, bias_out.astype(f32), w_first, w_short, w_rest, w_out.transpose(0, 1, 3, 2))
        return image.transpose(0, 3, 2, 1)

    return jax.shard_map(local_decode, mesh=mesh, in_specs=(tile_spec, replicated, replicated, replicated, replicated, replicated, replicated, replicated, replicated), out_specs=tile_spec, check_vma=False)
```

```python
import jax
import jax.numpy as jnp
from jax import lax
from jax.experimental import pallas as pl
from jax.experimental.pallas import tpu as pltpu
from jax.sharding import PartitionSpec as P

GROUPS = 32
GN_EPS = 1e-6
MESH = pl.DeviceIdType.MESH
BATCH = 3


def solution(mesh):
    rows_n = mesh.shape["sy"]
    cols_n = mesh.shape["sx"]
    tile_spec = P("dp", "sy", "sx", None)
    replicated = P()
    bf16 = jnp.bfloat16
    f32 = jnp.float32

    def make_kernel(samples, tile_h, tile_w):
        lanes = 16
        planes = tile_h // lanes
        ext_w = tile_w + 2
        pairs = planes // 2
        pixel_count = float(tile_h * rows_n * tile_w * cols_n)

        batches = samples // BATCH
        column_lanes = (planes + 2) * lanes
        flat_width = -(-(ext_w * column_lanes) // 128) * 128

        def kernel(act_hbm, norm_first, norm_rest, bias_rest, bias_out, w_first_hbm, w_short, w_rest_hbm, w_out, out_ref,
                   a_ext, t_ext, h_ext, a_ud, t_ud, h_ud, act_a0, act_a1, act_m0, act_m1, w_first, w_rest, wp_first, wp_rest, w_head, reorder, image_rows,
                   raw, rx1, rx2, rx1a, rx2a,
                   raw_sem, weight_sem, col_send, col_recv, row_send, row_recv, st1_send, st1_recv, st2_send, st2_recv):
            my_y = lax.axis_index("sy")
            my_x = lax.axis_index("sx")
            has_up = my_y > 0
            has_down = my_y < rows_n - 1
            has_left = my_x > 0
            has_right = my_x < cols_n - 1

            barrier = pltpu.get_barrier_semaphore()
            for step in range(1, rows_n * cols_n):
                other = lax.rem(my_y * cols_n + my_x + step, rows_n * cols_n)
                pl.semaphore_signal(barrier, inc=1, device_id={"sy": other // cols_n, "sx": lax.rem(other, cols_n)}, device_id_type=MESH)

            def fetch(sample):
                slot = lax.rem(sample, 2)
                return [pltpu.make_async_copy(act_hbm.at[sample, pl.ds(4 * part, 4)], raw.at[slot, pl.ds(4 * part, 4)], raw_sem.at[slot, part]) for part in range(lanes // 4)]

            first_in = pltpu.make_async_copy(w_first_hbm, w_first, weight_sem.at[0])
            rest_in = pltpu.make_async_copy(w_rest_hbm, w_rest, weight_sem.at[1])
            for copy in fetch(0):
                copy.start()
            first_in.start()
            rest_in.start()
            pl.semaphore_wait(barrier, rows_n * cols_n - 1)

            def pair_weights(dst, src, chans):
                for dc in range(3):
                    for j in range(4):
                        base = (dc * 4 + j) * chans
                        zero = jnp.zeros((chans, 128), bf16)
                        dst[pl.ds(base, chans), 0:128] = src(j, dc) if j < 3 else zero
                        dst[pl.ds(base, chans), 128:256] = src(j - 1, dc) if j > 0 else zero

            def span(batch):
                return pl.ds(batch * BATCH, BATCH)

            def remote(src, dst, send_sem, recv_sem, to_y, to_x):
                return pltpu.make_async_remote_copy(src_ref=src, dst_ref=dst, send_sem=send_sem, recv_sem=recv_sem,
                                                    device_id={"sy": to_y, "sx": to_x}, device_id_type=MESH)

            def sample_columns(layer, sample):
                ext, _, parity, _, _ = layer_out(layer)
                moves = [(has_left, has_right, 1, ext_w - 1, my_x - 1), (has_right, has_left, ext_w - 2, 0, my_x + 1)]
                return [(leaves, arrives, remote(ext.at[sample, :, src], ext.at[sample, :, dst], col_send.at[sample, index], col_recv.at[parity, sample, index], my_y, to_x))
                        for index, (leaves, arrives, src, dst, to_x) in enumerate(moves)]

            def column_copies(layer, batch):
                return [copy for index in range(BATCH) for copy in sample_columns(layer, batch * BATCH + index)]

            def row_copies(ext, ud, parity, batch):
                moves = [(has_up, has_down, 0, 1, my_y - 1), (has_down, has_up, planes - 1, 0, my_y + 1)]
                return [(leaves, arrives, remote(ext.at[span(batch), src], ud.at[side, span(batch)], row_send.at[batch, side], row_recv.at[parity, batch, side], to_y, my_x))
                        for leaves, arrives, src, side, to_y in moves]

            def peers(buf, send_sem, recv_sem, parity, batch, along_y):
                mine = my_y if along_y else my_x
                count = rows_n if along_y else cols_n
                copies = []
                for step in range(1, count):
                    to = lax.rem(mine + step, count)
                    slot = buf.at[parity, batch, mine]
                    copies.append(remote(slot, slot, send_sem.at[batch, step], recv_sem.at[parity, batch, step], to if along_y else my_y, my_x if along_y else to))
                return copies

            def layer_out(layer):
                if layer == 0:
                    return a_ext, a_ud, 0, rx1a, rx2a
                if layer % 2:
                    return t_ext, t_ud, 1, rx1, rx2
                return h_ext, h_ud, 0, rx1, rx2

            def start_if(cond, copy):
                @pl.when(cond)
                def _():
                    copy.start()

            def send_batch(layer, batch):
                if layer > 0:
                    for leaves, _, copy in column_copies(layer, batch):
                        start_if(leaves, copy)
                send_sums(layer, batch)

            def send_sums(layer, batch):
                _, _, parity, sums_one, _ = layer_out(layer)
                for copy in peers(sums_one, st1_send, st1_recv, parity, batch, True):
                    copy.start()

            def relay_rows(layer, batch):
                ext, ud, parity, _, _ = layer_out(layer)
                for _, arrives, copy in column_copies(layer, batch):
                    @pl.when(arrives)
                    def _(copy=copy):
                        copy.wait_recv()
                for leaves, _, copy in row_copies(ext, ud, parity, batch):
                    start_if(leaves, copy)

            def fold_sums(layer, batch):
                _, _, parity, sums_one, sums_two = layer_out(layer)
                for copy in peers(sums_one, st1_send, st1_recv, parity, batch, True):
                    copy.wait_recv()
                total = sums_one[parity, batch, 0]
                for index in range(1, rows_n):
                    total = total + sums_one[parity, batch, index]
                parts = 2 if layer == 0 else 1
                for index in range(BATCH):
                    sums_two[parity, batch, my_x, index] = pack_groups(total[index], parts)

            def send_totals(layer, batch):
                _, _, parity, _, sums_two = layer_out(layer)
                for copy in peers(sums_two, st2_send, st2_recv, parity, batch, False):
                    copy.start()

            def boundary(layer, batch):
                if layer < 7:
                    @pl.when(batch >= 2)
                    def _():
                        fold_sums(layer, batch - 2)

                    @pl.when(batch >= 3)
                    def _():
                        relay_rows(layer, batch - 3)

                if layer > 0:
                    @pl.when(batch < 2)
                    def _():
                        fold_sums(layer - 1, batches + batch - 2)

                    @pl.when(batch < 3)
                    def _():
                        relay_rows(layer - 1, batches + batch - 3)

                    @pl.when(batch < 2)
                    def _():
                        send_totals(layer - 1, batches + batch - 2)

                if layer < 7:
                    @pl.when(batch >= 2)
                    def _():
                        send_totals(layer, batch - 2)

                    @pl.when(batch > 0)
                    def _():
                        send_batch(layer, batch - 1)

            def await_batch(layer, batch):
                ext, ud, parity, sums_one, sums_two = layer_out(layer)
                rows = row_copies(ext, ud, parity, batch)
                for _, arrives, copy in rows:
                    @pl.when(arrives)
                    def _(copy=copy):
                        copy.wait_recv()
                for leaves, _, copy in rows:
                    @pl.when(leaves)
                    def _(copy=copy):
                        copy.wait_send()
                for leaves, _, copy in column_copies(layer, batch):
                    @pl.when(leaves)
                    def _(copy=copy):
                        copy.wait_send()
                for copy in peers(sums_one, st1_send, st1_recv, parity, batch, True):
                    copy.wait_send()
                for copy in peers(sums_two, st2_send, st2_recv, parity, batch, False):
                    copy.wait()

            def group_total(value, per_group):
                lane = lax.broadcasted_iota(jnp.int32, value.shape, 1)
                step = 1
                while step < per_group:
                    ahead = pltpu.roll(value, 128 - step, axis=1)
                    behind = pltpu.roll(value, step, axis=1)
                    value = value + jnp.where(lax.rem(lane, 2 * step) < step, ahead, behind)
                    step *= 2
                return value

            def pack_groups(sums, parts):
                rows = 2 * parts
                groups = group_total(sums, 128 * parts // GROUPS)
                lane = lax.rem(lax.broadcasted_iota(jnp.int32, (1, 128), 1), rows)
                packed = groups[0:1]
                for row in range(1, rows):
                    packed = jnp.where(lane == row, groups[row:row + 1], packed)
                return packed

            def unpack_groups(packed, parts):
                rows = 2 * parts
                lane = lax.rem(lax.broadcasted_iota(jnp.int32, (1, 128), 1), rows)
                return [group_total(jnp.where(lane == row, packed, 0.0), rows) for row in range(rows)]

            def scale_shift(layer, sample):
                _, _, parity, _, sums_two = layer_out(layer)
                batch, index = sample // BATCH, lax.rem(sample, BATCH)
                total = sums_two[parity, batch, 0, index]
                for source in range(1, cols_n):
                    total = total + sums_two[parity, batch, source, index]
                parts = 2 if layer == 0 else 1
                moments = unpack_groups(total * (1.0 / (pixel_count * (128 * parts // GROUPS))), parts)
                pair = (norm_first[...] if layer == 0 else norm_rest[layer - 1]).astype(f32)
                result = []
                for part in range(parts):
                    mean, square = moments[part], moments[parts + part]
                    inv = lax.rsqrt(square - mean * mean + GN_EPS)
                    scale = inv * pair[0:1, part * 128:(part + 1) * 128]
                    shift = pair[1:2, part * 128:(part + 1) * 128] - mean * scale
                    result.append((0.5 * scale, 0.5 * shift))
                if parts == 1:
                    return result[0]
                return tuple(jnp.concatenate([result[0][i], result[1][i]], axis=1) for i in range(2))

            half_planes = planes // 2

            def activate(layer, sample):
                ext, ud, _, _, _ = layer_out(layer)
                upper, lower = (act_a0, act_a1) if layer == 0 else (act_m0, act_m1)
                chans = 256 if layer == 0 else 128
                scale, shift = scale_shift(layer, sample)
                scale3 = scale.reshape(1, 1, chans)
                shift3 = shift.reshape(1, 1, chans)
                shape = (ext_w, lanes, chans)
                col_id = lax.broadcasted_iota(jnp.int32, shape, 0)
                row_id = lax.broadcasted_iota(jnp.int32, shape, 1)
                in_cols = (col_id >= jnp.where(has_left, 0, 1)) & (col_id <= jnp.where(has_right, ext_w - 1, ext_w - 2))

                def silu(x):
                    half = x.astype(f32) * scale3 + shift3
                    return half + half * jnp.tanh(half)

                def put(plane, cols, value):
                    if plane <= half_planes + 1:
                        upper[plane // 2, plane % 2, cols] = value
                    if plane >= half_planes:
                        lower[(plane - half_planes) // 2, plane % 2, cols] = value

                def tile_plane(q):
                    put(q + 1, pl.ds(1, tile_w), silu(ext[sample, q, pl.ds(1, tile_w)]).astype(bf16))
                    for col, cond in ((0, has_left), (ext_w - 1, has_right)):
                        put(q + 1, pl.ds(col, 1), jnp.where(cond, silu(ext[sample, q, pl.ds(col, 1)]), 0.0).astype(bf16))

                def border_plane(near, plane, side, cond, turn, edge):
                    own = pltpu.roll(jnp.where(in_cols, silu(ext[sample, near]), 0.0), turn, axis=1)
                    other = pltpu.roll(jnp.where(in_cols & cond, silu(ud[side, sample]), 0.0), turn, axis=1)
                    put(plane, slice(None), jnp.where(row_id == edge, other, own).astype(bf16))

                def fill_upper():
                    border_plane(planes - 1, 0, 0, has_up, 1, 0)
                    for q in range(half_planes + 1):
                        tile_plane(q)

                def fill_lower():
                    for q in range(half_planes + 1, planes):
                        tile_plane(q)
                    border_plane(0, planes + 1, 1, has_down, lanes - 1, lanes - 1)

                return fill_upper, fill_lower

            def activate_convolve(layer, sample):
                fill_upper, fill_lower = activate(layer - 1, sample)
                chans = 256 if layer == 1 else 128
                ext, _, parity, sums_one, _ = layer_out(layer)
                bias_rows = bias_rest[...].astype(f32)
                bias = bias_rows[layer - 1:layer]
                if layer == 2:
                    bias = bias + bias_rows[6:7]
                weights = wp_first if layer == 1 else wp_rest.at[layer - 2]
                sums = [jnp.zeros((8, 128), f32), jnp.zeros((8, 128), f32)]
                parts = 4
                share = pairs // parts

                def product(part):
                    src = ((act_a0, act_a1) if layer == 1 else (act_m0, act_m1))[part // 2]
                    base = part % 2 * share
                    pieces = [src[pl.ds(base + j // 2, share), j % 2, pl.ds(dc, tile_w)].reshape(share * tile_w * lanes, chans) for dc in range(3) for j in range(4)]
                    return jnp.dot(jnp.concatenate(pieces, axis=1), weights[...], preferred_element_type=f32)

                def finish(part, accum):
                    for k in range(share):
                        for odd in range(2):
                            q = 2 * (part * share + k) + odd
                            value = accum[k * 128:(k + 1) * 128, odd * 128:(odd + 1) * 128].reshape(tile_w, lanes, 128) + bias.reshape(1, 1, 128)
                            if layer == 2:
                                skip = jnp.dot(a_ext[sample, q, pl.ds(1, tile_w)].reshape(128, 256), w_short[...], preferred_element_type=f32)
                                value = value + skip.reshape(tile_w, lanes, 128)
                            elif layer % 2 == 0:
                                value = value + ext[sample, q, pl.ds(1, tile_w)].astype(f32)
                            value = value.astype(bf16)
                            ext[sample, q, pl.ds(1, tile_w)] = value
                            wide = value.astype(f32).reshape(tile_w * 2, 8, 128)
                            sums[0] = sums[0] + jnp.sum(wide, axis=0)
                            sums[1] = sums[1] + jnp.sum(wide * wide, axis=0)

                fill_upper()
                first = [product(0), product(1)]
                fill_lower()
                for part in range(2):
                    finish(part, first[part])
                second = [product(2), product(3)]
                for part in range(2):
                    finish(2 + part, second[part])
                sums_one[parity, sample // BATCH, my_y, lax.rem(sample, BATCH)] = jnp.concatenate(
                    [jnp.sum(sums[0], axis=0, keepdims=True), jnp.sum(sums[1], axis=0, keepdims=True)], axis=0)

            def load_step(index, batch):
                sample = batch * BATCH + index

                @pl.when(sample > 0)
                def _():
                    for leaves, _, copy in sample_columns(0, sample - 1):
                        start_if(leaves, copy)

                @pl.when(sample + 1 < samples)
                def _():
                    for copy in fetch(sample + 1):
                        copy.start()

                for copy in fetch(sample):
                    copy.wait()
                slot = lax.rem(sample, 2)
                sum_one = jnp.zeros((8, 256), f32)
                sum_two = jnp.zeros((8, 256), f32)
                for q in range(planes):
                    value = jnp.swapaxes(raw[slot, :, q].astype(f32), 0, 1)
                    a_ext[sample, q, pl.ds(1, tile_w)] = value.astype(bf16)
                    wide = value.reshape(2 * tile_w, 8, 256)
                    sum_one = sum_one + jnp.sum(wide, axis=0)
                    sum_two = sum_two + jnp.sum(wide * wide, axis=0)
                one = jnp.sum(sum_one, axis=0, keepdims=True)
                two = jnp.sum(sum_two, axis=0, keepdims=True)
                rx1a[0, batch, my_y, index] = jnp.concatenate([one[:, :128], one[:, 128:], two[:, :128], two[:, 128:]], axis=0)
                return batch

            def load_batch(batch, carry):
                boundary(0, batch)
                lax.fori_loop(0, BATCH, load_step, batch)
                return carry

            lax.fori_loop(0, batches, load_batch, 0)
            for leaves, _, copy in sample_columns(0, samples - 1):
                start_if(leaves, copy)
            send_batch(0, batches - 1)

            first_in.wait()
            rest_in.wait()
            pair_weights(wp_first, lambda dr, dc: w_first[dr, dc], 256)

            def pair_rest(index, carry):
                pair_weights(wp_rest.at[index], lambda dr, dc: w_rest[index, dr, dc], 128)
                return carry

            lax.fori_loop(0, 5, pair_rest, 0)

            for tap in range(9):
                taps3 = w_out[tap // 3, tap % 3].astype(f32)
                w_head[pl.ds(8 * tap, 8), :] = jnp.concatenate([taps3, jnp.zeros((5, 128), f32)], axis=0)
            from_id = lax.broadcasted_iota(jnp.int32, (tile_h, tile_h), 0)
            to_id = lax.broadcasted_iota(jnp.int32, (tile_h, tile_h), 1)
            reorder[...] = jnp.where(lax.rem(from_id, lanes) * planes + from_id // lanes == to_id, 1.0, 0.0).astype(bf16)

            for layer in range(1, 7):
                def conv_step(index, batch, layer=layer):
                    activate_convolve(layer, batch * BATCH + index)
                    return batch

                def conv_batch(batch, carry, layer=layer, conv_step=conv_step):
                    boundary(layer, batch)
                    await_batch(layer - 1, batch)
                    lax.fori_loop(0, BATCH, conv_step, batch)
                    return carry

                lax.fori_loop(0, batches, conv_batch, 0)
                send_batch(layer, batches - 1)

            def head_step(index, batch):
                sample = batch * BATCH + index

                for fill in activate(6, sample):
                    fill()
                rows = half_planes + 2
                flat = jnp.concatenate([act_m0[...].reshape(rows, ext_w, lanes, 128), act_m1[...].reshape(rows, ext_w, lanes, 128)[2:]], axis=0)
                flat = jnp.swapaxes(flat, 0, 1).reshape(ext_w * column_lanes, 128)
                flat = jnp.concatenate([flat, jnp.zeros((flat_width - flat.shape[0], 128), bf16)], axis=0)
                taps = lax.dot_general(w_head[...].astype(bf16), flat, (((1,), (1,)), ((), ())), preferred_element_type=f32)
                image = taps[0:8]
                for tap in range(1, 9):
                    offset = (tap % 3) * column_lanes + (tap // 3) * lanes
                    image = image + pltpu.roll(taps[8 * tap:8 * tap + 8], flat_width - offset, axis=1)
                rest = jnp.concatenate([image[:, c * column_lanes:c * column_lanes + tile_h] for c in range(tile_w)], axis=0)
                moved = jnp.zeros(rest.shape, f32)
                for _ in range(3):
                    piece = rest.astype(bf16)
                    moved = moved + jnp.dot(piece, reorder[...], preferred_element_type=f32)
                    rest = rest - piece.astype(f32)
                for side in range(tile_h // 128):
                    image_rows[side] = moved[:, side * 128:(side + 1) * 128]
                for chan in range(3):
                    for side in range(tile_h // 128):
                        out_ref[sample, chan, :, side * 128:(side + 1) * 128] = image_rows[side, pl.ds(chan, tile_w, stride=8), :] + bias_out[chan]
                return batch

            def head_batch(batch, carry):
                boundary(7, batch)
                await_batch(6, batch)
                lax.fori_loop(0, BATCH, head_step, batch)
                return carry

            lax.fori_loop(0, batches, head_batch, 0)

        return kernel, lanes, planes, ext_w

    def local_decode(act_in, norm_first, w_first, w_short, norm_rest, w_rest, bias_rest, w_out, bias_out):
        samples, tile_h, tile_w, _ = act_in.shape
        kernel, lanes, planes, ext_w = make_kernel(samples, tile_h, tile_w)
        batches = samples // BATCH
        vmem = pl.BlockSpec(memory_space=pltpu.VMEM)
        hbm = pl.BlockSpec(memory_space=pl.ANY)
        scratch = [
            pltpu.VMEM((samples, planes, ext_w, lanes, 256), bf16),
            pltpu.VMEM((samples, planes, ext_w, lanes, 128), bf16),
            pltpu.VMEM((samples, planes, ext_w, lanes, 128), bf16),
            pltpu.VMEM((2, samples, ext_w, lanes, 256), bf16),
            pltpu.VMEM((2, samples, ext_w, lanes, 128), bf16),
            pltpu.VMEM((2, samples, ext_w, lanes, 128), bf16),
            pltpu.VMEM((planes // 4 + 1, 2, ext_w, lanes, 256), bf16),
            pltpu.VMEM((planes // 4 + 1, 2, ext_w, lanes, 256), bf16),
            pltpu.VMEM((planes // 4 + 1, 2, ext_w, lanes, 128), bf16),
            pltpu.VMEM((planes // 4 + 1, 2, ext_w, lanes, 128), bf16),
            pltpu.VMEM((3, 3, 256, 128), bf16),
            pltpu.VMEM((5, 3, 3, 128, 128), bf16),
            pltpu.VMEM((12 * 256, 256), bf16),
            pltpu.VMEM((5, 12 * 128, 256), bf16),
            pltpu.VMEM((72, 128), f32),
            pltpu.VMEM((tile_h, tile_h), bf16),
            pltpu.VMEM((tile_h // 128, 8 * tile_w, 128), f32),
            pltpu.VMEM((2, lanes, planes, tile_w, 256), bf16),
            pltpu.VMEM((2, batches, rows_n, BATCH, 2, 128), f32),
            pltpu.VMEM((2, batches, cols_n, BATCH, 1, 128), f32),
            pltpu.VMEM((1, batches, rows_n, BATCH, 4, 128), f32),
            pltpu.VMEM((1, batches, cols_n, BATCH, 1, 128), f32),
            pltpu.SemaphoreType.DMA((2, lanes // 4)),
            pltpu.SemaphoreType.DMA((2,)),
            pltpu.SemaphoreType.DMA((samples, 2)),
            pltpu.SemaphoreType.DMA((2, samples, 2)),
            pltpu.SemaphoreType.DMA((batches, 2)),
            pltpu.SemaphoreType.DMA((2, batches, 2)),
            pltpu.SemaphoreType.DMA((batches, rows_n)),
            pltpu.SemaphoreType.DMA((2, batches, rows_n)),
            pltpu.SemaphoreType.DMA((batches, cols_n)),
            pltpu.SemaphoreType.DMA((2, batches, cols_n)),
        ]
        image = pl.pallas_call(
            kernel,
            out_shape=jax.ShapeDtypeStruct((samples, 3, tile_w, tile_h), f32),
            in_specs=[hbm, vmem, vmem, vmem, pl.BlockSpec(memory_space=pltpu.SMEM), hbm, vmem, hbm, vmem],
            out_specs=vmem,
            scratch_shapes=scratch,
            compiler_params=pltpu.CompilerParams(collective_id=0, has_side_effects=True, vmem_limit_bytes=60 * 1024 * 1024),
        )(act_in.reshape(samples, lanes, planes, tile_w, 256), norm_first, norm_rest, bias_rest, bias_out.astype(f32), w_first, w_short, w_rest, w_out.transpose(0, 1, 3, 2))
        return image.transpose(0, 3, 2, 1)

    return jax.shard_map(local_decode, mesh=mesh, in_specs=(tile_spec, replicated, replicated, replicated, replicated, replicated, replicated, replicated, replicated), out_specs=tile_spec, check_vma=False)
```

```python
import jax
import jax.numpy as jnp
from jax import lax
from jax.experimental import pallas as pl
from jax.experimental.pallas import tpu as pltpu
from jax.sharding import PartitionSpec as P

GROUPS = 32
GN_EPS = 1e-6
MESH = pl.DeviceIdType.MESH
BATCH = 3


def solution(mesh):
    rows_n = mesh.shape["sy"]
    cols_n = mesh.shape["sx"]
    tile_spec = P("dp", "sy", "sx", None)
    replicated = P()
    bf16 = jnp.bfloat16
    f32 = jnp.float32

    def make_kernel(samples, tile_h, tile_w):
        lanes = 16
        planes = tile_h // lanes
        ext_w = tile_w + 2
        pairs = planes // 2
        pixel_count = float(tile_h * rows_n * tile_w * cols_n)

        batches = samples // BATCH
        column_lanes = (planes + 2) * lanes
        flat_width = -(-(ext_w * column_lanes) // 128) * 128

        def kernel(act_hbm, norm_first, norm_rest, bias_rest, bias_out, w_first_hbm, w_short, w_rest_hbm, w_out, out_ref,
                   a_ext, t_ext, h_ext, a_ud, t_ud, h_ud, act_a0, act_a1, act_m0, act_m1, w_first, w_rest, wp_first, wp_rest, w_head, reorder, image_rows,
                   raw, rx1, rx2, rx1a, rx2a,
                   raw_sem, weight_sem, col_send, col_recv, row_send, row_recv, st1_send, st1_recv, st2_send, st2_recv):
            my_y = lax.axis_index("sy")
            my_x = lax.axis_index("sx")
            has_up = my_y > 0
            has_down = my_y < rows_n - 1
            has_left = my_x > 0
            has_right = my_x < cols_n - 1

            barrier = pltpu.get_barrier_semaphore()
            for step in range(1, rows_n * cols_n):
                other = lax.rem(my_y * cols_n + my_x + step, rows_n * cols_n)
                pl.semaphore_signal(barrier, inc=1, device_id={"sy": other // cols_n, "sx": lax.rem(other, cols_n)}, device_id_type=MESH)

            def fetch(sample):
                slot = lax.rem(sample, 2)
                return [pltpu.make_async_copy(act_hbm.at[sample, pl.ds(4 * part, 4)], raw.at[slot, pl.ds(4 * part, 4)], raw_sem.at[slot, part]) for part in range(lanes // 4)]

            first_in = pltpu.make_async_copy(w_first_hbm, w_first, weight_sem.at[0])
            rest_in = pltpu.make_async_copy(w_rest_hbm, w_rest, weight_sem.at[1])
            for copy in fetch(0):
                copy.start()
            first_in.start()
            rest_in.start()
            pl.semaphore_wait(barrier, rows_n * cols_n - 1)

            def pair_weights(dst, src, chans):
                for dc in range(3):
                    for j in range(4):
                        base = (dc * 4 + j) * chans
                        zero = jnp.zeros((chans, 128), bf16)
                        dst[pl.ds(base, chans), 0:128] = src(j, dc) if j < 3 else zero
                        dst[pl.ds(base, chans), 128:256] = src(j - 1, dc) if j > 0 else zero

            def span(batch):
                return pl.ds(batch * BATCH, BATCH)

            def remote(src, dst, send_sem, recv_sem, to_y, to_x):
                return pltpu.make_async_remote_copy(src_ref=src, dst_ref=dst, send_sem=send_sem, recv_sem=recv_sem,
                                                    device_id={"sy": to_y, "sx": to_x}, device_id_type=MESH)

            def sample_columns(layer, sample):
                ext, _, parity, _, _ = layer_out(layer)
                moves = [(has_left, has_right, 1, ext_w - 1, my_x - 1), (has_right, has_left, ext_w - 2, 0, my_x + 1)]
                return [(leaves, arrives, remote(ext.at[sample, :, src], ext.at[sample, :, dst], col_send.at[sample, index], col_recv.at[parity, sample, index], my_y, to_x))
                        for index, (leaves, arrives, src, dst, to_x) in enumerate(moves)]

            def column_copies(layer, batch):
                return [copy for index in range(BATCH) for copy in sample_columns(layer, batch * BATCH + index)]

            def row_copies(ext, ud, parity, batch):
                moves = [(has_up, has_down, 0, 1, my_y - 1), (has_down, has_up, planes - 1, 0, my_y + 1)]
                return [(leaves, arrives, remote(ext.at[span(batch), src], ud.at[side, span(batch)], row_send.at[batch, side], row_recv.at[parity, batch, side], to_y, my_x))
                        for leaves, arrives, src, side, to_y in moves]

            def peers(buf, send_sem, recv_sem, parity, batch, along_y):
                mine = my_y if along_y else my_x
                count = rows_n if along_y else cols_n
                copies = []
                for step in range(1, count):
                    to = lax.rem(mine + step, count)
                    slot = buf.at[parity, batch, mine]
                    copies.append(remote(slot, slot, send_sem.at[batch, step], recv_sem.at[parity, batch, step], to if along_y else my_y, my_x if along_y else to))
                return copies

            def layer_out(layer):
                if layer == 0:
                    return a_ext, a_ud, 0, rx1a, rx2a
                if layer % 2:
                    return t_ext, t_ud, 1, rx1, rx2
                return h_ext, h_ud, 0, rx1, rx2

            def start_if(cond, copy):
                @pl.when(cond)
                def _():
                    copy.start()

            def send_batch(layer, batch):
                if layer > 0:
                    for leaves, _, copy in column_copies(layer, batch):
                        start_if(leaves, copy)
                send_sums(layer, batch)

            def send_sums(layer, batch):
                _, _, parity, sums_one, _ = layer_out(layer)
                for copy in peers(sums_one, st1_send, st1_recv, parity, batch, True):
                    copy.start()

            def relay_rows(layer, batch):
                ext, ud, parity, _, _ = layer_out(layer)
                for _, arrives, copy in column_copies(layer, batch):
                    @pl.when(arrives)
                    def _(copy=copy):
                        copy.wait_recv()
                for leaves, _, copy in row_copies(ext, ud, parity, batch):
                    start_if(leaves, copy)

            def fold_sums(layer, batch):
                _, _, parity, sums_one, sums_two = layer_out(layer)
                for copy in peers(sums_one, st1_send, st1_recv, parity, batch, True):
                    copy.wait_recv()
                total = sums_one[parity, batch, 0]
                for index in range(1, rows_n):
                    total = total + sums_one[parity, batch, index]
                parts = 2 if layer == 0 else 1
                for index in range(BATCH):
                    sums_two[parity, batch, my_x, index] = pack_groups(total[index], parts)

            def send_totals(layer, batch):
                _, _, parity, _, sums_two = layer_out(layer)
                for copy in peers(sums_two, st2_send, st2_recv, parity, batch, False):
                    copy.start()

            def boundary(layer, batch):
                if layer < 7:
                    @pl.when(batch >= 2)
                    def _():
                        fold_sums(layer, batch - 2)

                    @pl.when(batch >= 3)
                    def _():
                        relay_rows(layer, batch - 3)

                if layer > 0:
                    @pl.when(batch < 2)
                    def _():
                        fold_sums(layer - 1, batches + batch - 2)

                    @pl.when(batch < 3)
                    def _():
                        relay_rows(layer - 1, batches + batch - 3)

                    @pl.when(batch < 2)
                    def _():
                        send_totals(layer - 1, batches + batch - 2)

                    @pl.when(batch == 0)
                    def _():
                        send_batch(layer - 1, batches - 1)

                if layer < 7:
                    @pl.when(batch >= 2)
                    def _():
                        send_totals(layer, batch - 2)

                    @pl.when(batch > 0)
                    def _():
                        send_batch(layer, batch - 1)

            def await_batch(layer, batch):
                ext, ud, parity, sums_one, sums_two = layer_out(layer)
                rows = row_copies(ext, ud, parity, batch)
                for _, arrives, copy in rows:
                    @pl.when(arrives)
                    def _(copy=copy):
                        copy.wait_recv()
                for leaves, _, copy in rows:
                    @pl.when(leaves)
                    def _(copy=copy):
                        copy.wait_send()
                for leaves, _, copy in column_copies(layer, batch):
                    @pl.when(leaves)
                    def _(copy=copy):
                        copy.wait_send()
                for copy in peers(sums_one, st1_send, st1_recv, parity, batch, True):
                    copy.wait_send()
                for copy in peers(sums_two, st2_send, st2_recv, parity, batch, False):
                    copy.wait()

            def group_total(value, per_group):
                lane = lax.broadcasted_iota(jnp.int32, value.shape, 1)
                step = 1
                while step < per_group:
                    ahead = pltpu.roll(value, 128 - step, axis=1)
                    behind = pltpu.roll(value, step, axis=1)
                    value = value + jnp.where(lax.rem(lane, 2 * step) < step, ahead, behind)
                    step *= 2
                return value

            def pack_groups(sums, parts):
                rows = 2 * parts
                groups = group_total(sums, 128 * parts // GROUPS)
                lane = lax.rem(lax.broadcasted_iota(jnp.int32, (1, 128), 1), rows)
                packed = groups[0:1]
                for row in range(1, rows):
                    packed = jnp.where(lane == row, groups[row:row + 1], packed)
                return packed

            def unpack_groups(packed, parts):
                rows = 2 * parts
                lane = lax.rem(lax.broadcasted_iota(jnp.int32, (1, 128), 1), rows)
                return [group_total(jnp.where(lane == row, packed, 0.0), rows) for row in range(rows)]

            def scale_shift(layer, sample):
                _, _, parity, _, sums_two = layer_out(layer)
                batch, index = sample // BATCH, lax.rem(sample, BATCH)
                total = sums_two[parity, batch, 0, index]
                for source in range(1, cols_n):
                    total = total + sums_two[parity, batch, source, index]
                parts = 2 if layer == 0 else 1
                moments = unpack_groups(total * (1.0 / (pixel_count * (128 * parts // GROUPS))), parts)
                pair = (norm_first[...] if layer == 0 else norm_rest[layer - 1]).astype(f32)
                result = []
                for part in range(parts):
                    mean, square = moments[part], moments[parts + part]
                    inv = lax.rsqrt(square - mean * mean + GN_EPS)
                    scale = inv * pair[0:1, part * 128:(part + 1) * 128]
                    shift = pair[1:2, part * 128:(part + 1) * 128] - mean * scale
                    result.append((0.5 * scale, 0.5 * shift))
                if parts == 1:
                    return result[0]
                return tuple(jnp.concatenate([result[0][i], result[1][i]], axis=1) for i in range(2))

            half_planes = planes // 2

            def activate(layer, sample):
                ext, ud, _, _, _ = layer_out(layer)
                upper, lower = (act_a0, act_a1) if layer == 0 else (act_m0, act_m1)
                chans = 256 if layer == 0 else 128
                scale, shift = scale_shift(layer, sample)
                scale3 = scale.reshape(1, 1, chans)
                shift3 = shift.reshape(1, 1, chans)
                shape = (ext_w, lanes, chans)
                col_id = lax.broadcasted_iota(jnp.int32, shape, 0)
                row_id = lax.broadcasted_iota(jnp.int32, shape, 1)
                in_cols = (col_id >= jnp.where(has_left, 0, 1)) & (col_id <= jnp.where(has_right, ext_w - 1, ext_w - 2))

                def silu(x):
                    half = x.astype(f32) * scale3 + shift3
                    return half + half * jnp.tanh(half)

                def put(plane, cols, value):
                    if plane <= half_planes + 1:
                        upper[plane // 2, plane % 2, cols] = value
                    if plane >= half_planes:
                        lower[(plane - half_planes) // 2, plane % 2, cols] = value

                def tile_plane(q):
                    put(q + 1, pl.ds(1, tile_w), silu(ext[sample, q, pl.ds(1, tile_w)]).astype(bf16))
                    for col, cond in ((0, has_left), (ext_w - 1, has_right)):
                        put(q + 1, pl.ds(col, 1), jnp.where(cond, silu(ext[sample, q, pl.ds(col, 1)]), 0.0).astype(bf16))

                def border_plane(near, plane, side, cond, turn, edge):
                    own = pltpu.roll(jnp.where(in_cols, silu(ext[sample, near]), 0.0), turn, axis=1)
                    other = pltpu.roll(jnp.where(in_cols & cond, silu(ud[side, sample]), 0.0), turn, axis=1)
                    put(plane, slice(None), jnp.where(row_id == edge, other, own).astype(bf16))

                def fill_upper():
                    border_plane(planes - 1, 0, 0, has_up, 1, 0)
                    for q in range(half_planes + 1):
                        tile_plane(q)

                def fill_lower():
                    for q in range(half_planes + 1, planes):
                        tile_plane(q)
                    border_plane(0, planes + 1, 1, has_down, lanes - 1, lanes - 1)

                return fill_upper, fill_lower

            def activate_convolve(layer, sample):
                fill_upper, fill_lower = activate(layer - 1, sample)
                chans = 256 if layer == 1 else 128
                ext, _, parity, sums_one, _ = layer_out(layer)
                bias_rows = bias_rest[...].astype(f32)
                bias = bias_rows[layer - 1:layer]
                if layer == 2:
                    bias = bias + bias_rows[6:7]
                weights = wp_first if layer == 1 else wp_rest.at[layer - 2]
                sums = [jnp.zeros((8, 128), f32), jnp.zeros((8, 128), f32)]
                parts = 4
                share = pairs // parts

                def product(part):
                    src = ((act_a0, act_a1) if layer == 1 else (act_m0, act_m1))[part // 2]
                    base = part % 2 * share
                    pieces = [src[pl.ds(base + j // 2, share), j % 2, pl.ds(dc, tile_w)].reshape(share * tile_w * lanes, chans) for dc in range(3) for j in range(4)]
                    return jnp.dot(jnp.concatenate(pieces, axis=1), weights[...], preferred_element_type=f32)

                def finish(part, accum):
                    for k in range(share):
                        for odd in range(2):
                            q = 2 * (part * share + k) + odd
                            value = accum[k * 128:(k + 1) * 128, odd * 128:(odd + 1) * 128].reshape(tile_w, lanes, 128) + bias.reshape(1, 1, 128)
                            if layer == 2:
                                skip = jnp.dot(a_ext[sample, q, pl.ds(1, tile_w)].reshape(128, 256), w_short[...], preferred_element_type=f32)
                                value = value + skip.reshape(tile_w, lanes, 128)
                            elif layer % 2 == 0:
                                value = value + ext[sample, q, pl.ds(1, tile_w)].astype(f32)
                            value = value.astype(bf16)
                            ext[sample, q, pl.ds(1, tile_w)] = value
                            wide = value.astype(f32).reshape(tile_w * 2, 8, 128)
                            sums[0] = sums[0] + jnp.sum(wide, axis=0)
                            sums[1] = sums[1] + jnp.sum(wide * wide, axis=0)

                fill_upper()
                first = [product(0), product(1)]
                fill_lower()
                for part in range(2):
                    finish(part, first[part])
                second = [product(2), product(3)]
                for part in range(2):
                    finish(2 + part, second[part])
                sums_one[parity, sample // BATCH, my_y, lax.rem(sample, BATCH)] = jnp.concatenate(
                    [jnp.sum(sums[0], axis=0, keepdims=True), jnp.sum(sums[1], axis=0, keepdims=True)], axis=0)

            def load_step(index, batch):
                sample = batch * BATCH + index

                @pl.when(sample > 0)
                def _():
                    for leaves, _, copy in sample_columns(0, sample - 1):
                        start_if(leaves, copy)

                @pl.when(sample + 1 < samples)
                def _():
                    for copy in fetch(sample + 1):
                        copy.start()

                for copy in fetch(sample):
                    copy.wait()
                slot = lax.rem(sample, 2)
                sum_one = jnp.zeros((8, 256), f32)
                sum_two = jnp.zeros((8, 256), f32)
                for q in range(planes):
                    value = jnp.swapaxes(raw[slot, :, q].astype(f32), 0, 1)
                    a_ext[sample, q, pl.ds(1, tile_w)] = value.astype(bf16)
                    wide = value.reshape(2 * tile_w, 8, 256)
                    sum_one = sum_one + jnp.sum(wide, axis=0)
                    sum_two = sum_two + jnp.sum(wide * wide, axis=0)
                one = jnp.sum(sum_one, axis=0, keepdims=True)
                two = jnp.sum(sum_two, axis=0, keepdims=True)
                rx1a[0, batch, my_y, index] = jnp.concatenate([one[:, :128], one[:, 128:], two[:, :128], two[:, 128:]], axis=0)
                return batch

            def load_batch(batch, carry):
                boundary(0, batch)
                lax.fori_loop(0, BATCH, load_step, batch)
                return carry

            lax.fori_loop(0, batches, load_batch, 0)
            for leaves, _, copy in sample_columns(0, samples - 1):
                start_if(leaves, copy)

            first_in.wait()
            rest_in.wait()
            pair_weights(wp_first, lambda dr, dc: w_first[dr, dc], 256)

            def pair_rest(index, carry):
                pair_weights(wp_rest.at[index], lambda dr, dc: w_rest[index, dr, dc], 128)
                return carry

            lax.fori_loop(0, 5, pair_rest, 0)

            for tap in range(9):
                taps3 = w_out[tap // 3, tap % 3].astype(f32)
                w_head[pl.ds(8 * tap, 8), :] = jnp.concatenate([taps3, jnp.zeros((5, 128), f32)], axis=0)
            from_id = lax.broadcasted_iota(jnp.int32, (tile_h, tile_h), 0)
            to_id = lax.broadcasted_iota(jnp.int32, (tile_h, tile_h), 1)
            reorder[...] = jnp.where(lax.rem(from_id, lanes) * planes + from_id // lanes == to_id, 1.0, 0.0).astype(bf16)

            for layer in range(1, 7):
                def conv_step(index, batch, layer=layer):
                    activate_convolve(layer, batch * BATCH + index)
                    return batch

                def conv_batch(batch, carry, layer=layer, conv_step=conv_step):
                    boundary(layer, batch)
                    await_batch(layer - 1, batch)
                    lax.fori_loop(0, BATCH, conv_step, batch)
                    return carry

                lax.fori_loop(0, batches, conv_batch, 0)

            def head_step(index, batch):
                sample = batch * BATCH + index

                for fill in activate(6, sample):
                    fill()
                rows = half_planes + 2
                flat = jnp.concatenate([act_m0[...].reshape(rows, ext_w, lanes, 128), act_m1[...].reshape(rows, ext_w, lanes, 128)[2:]], axis=0)
                flat = jnp.swapaxes(flat, 0, 1).reshape(ext_w * column_lanes, 128)
                flat = jnp.concatenate([flat, jnp.zeros((flat_width - flat.shape[0], 128), bf16)], axis=0)
                taps = lax.dot_general(w_head[...].astype(bf16), flat, (((1,), (1,)), ((), ())), preferred_element_type=f32)
                image = taps[0:8]
                for tap in range(1, 9):
                    offset = (tap % 3) * column_lanes + (tap // 3) * lanes
                    image = image + pltpu.roll(taps[8 * tap:8 * tap + 8], flat_width - offset, axis=1)
                rest = jnp.concatenate([image[:, c * column_lanes:c * column_lanes + tile_h] for c in range(tile_w)], axis=0)
                moved = jnp.zeros(rest.shape, f32)
                for _ in range(3):
                    piece = rest.astype(bf16)
                    moved = moved + jnp.dot(piece, reorder[...], preferred_element_type=f32)
                    rest = rest - piece.astype(f32)
                for side in range(tile_h // 128):
                    image_rows[side] = moved[:, side * 128:(side + 1) * 128]
                for chan in range(3):
                    for side in range(tile_h // 128):
                        out_ref[sample, chan, :, side * 128:(side + 1) * 128] = image_rows[side, pl.ds(chan, tile_w, stride=8), :] + bias_out[chan]
                return batch

            def head_batch(batch, carry):
                boundary(7, batch)
                await_batch(6, batch)
                lax.fori_loop(0, BATCH, head_step, batch)
                return carry

            lax.fori_loop(0, batches, head_batch, 0)

        return kernel, lanes, planes, ext_w

    def local_decode(act_in, norm_first, w_first, w_short, norm_rest, w_rest, bias_rest, w_out, bias_out):
        samples, tile_h, tile_w, _ = act_in.shape
        kernel, lanes, planes, ext_w = make_kernel(samples, tile_h, tile_w)
        batches = samples // BATCH
        vmem = pl.BlockSpec(memory_space=pltpu.VMEM)
        hbm = pl.BlockSpec(memory_space=pl.ANY)
        scratch = [
            pltpu.VMEM((samples, planes, ext_w, lanes, 256), bf16),
            pltpu.VMEM((samples, planes, ext_w, lanes, 128), bf16),
            pltpu.VMEM((samples, planes, ext_w, lanes, 128), bf16),
            pltpu.VMEM((2, samples, ext_w, lanes, 256), bf16),
            pltpu.VMEM((2, samples, ext_w, lanes, 128), bf16),
            pltpu.VMEM((2, samples, ext_w, lanes, 128), bf16),
            pltpu.VMEM((planes // 4 + 1, 2, ext_w, lanes, 256), bf16),
            pltpu.VMEM((planes // 4 + 1, 2, ext_w, lanes, 256), bf16),
            pltpu.VMEM((planes // 4 + 1, 2, ext_w, lanes, 128), bf16),
            pltpu.VMEM((planes // 4 + 1, 2, ext_w, lanes, 128), bf16),
            pltpu.VMEM((3, 3, 256, 128), bf16),
            pltpu.VMEM((5, 3, 3, 128, 128), bf16),
            pltpu.VMEM((12 * 256, 256), bf16),
            pltpu.VMEM((5, 12 * 128, 256), bf16),
            pltpu.VMEM((72, 128), f32),
            pltpu.VMEM((tile_h, tile_h), bf16),
            pltpu.VMEM((tile_h // 128, 8 * tile_w, 128), f32),
            pltpu.VMEM((2, lanes, planes, tile_w, 256), bf16),
            pltpu.VMEM((2, batches, rows_n, BATCH, 2, 128), f32),
            pltpu.VMEM((2, batches, cols_n, BATCH, 1, 128), f32),
            pltpu.VMEM((1, batches, rows_n, BATCH, 4, 128), f32),
            pltpu.VMEM((1, batches, cols_n, BATCH, 1, 128), f32),
            pltpu.SemaphoreType.DMA((2, lanes // 4)),
            pltpu.SemaphoreType.DMA((2,)),
            pltpu.SemaphoreType.DMA((samples, 2)),
            pltpu.SemaphoreType.DMA((2, samples, 2)),
            pltpu.SemaphoreType.DMA((batches, 2)),
            pltpu.SemaphoreType.DMA((2, batches, 2)),
            pltpu.SemaphoreType.DMA((batches, rows_n)),
            pltpu.SemaphoreType.DMA((2, batches, rows_n)),
            pltpu.SemaphoreType.DMA((batches, cols_n)),
            pltpu.SemaphoreType.DMA((2, batches, cols_n)),
        ]
        image = pl.pallas_call(
            kernel,
            out_shape=jax.ShapeDtypeStruct((samples, 3, tile_w, tile_h), f32),
            in_specs=[hbm, vmem, vmem, vmem, pl.BlockSpec(memory_space=pltpu.SMEM), hbm, vmem, hbm, vmem],
            out_specs=vmem,
            scratch_shapes=scratch,
            compiler_params=pltpu.CompilerParams(collective_id=0, has_side_effects=True, vmem_limit_bytes=60 * 1024 * 1024),
        )(act_in.reshape(samples, lanes, planes, tile_w, 256), norm_first, norm_rest, bias_rest, bias_out.astype(f32), w_first, w_short, w_rest, w_out.transpose(0, 1, 3, 2))
        return image.transpose(0, 3, 2, 1)

    return jax.shard_map(local_decode, mesh=mesh, in_specs=(tile_spec, replicated, replicated, replicated, replicated, replicated, replicated, replicated, replicated), out_specs=tile_spec, check_vma=False)
```
